128 devices in a mesh: dp: 16 (over z, y), tp: 8 (over x, core).
Axes of the slice: x: 4, y: 4, z: 4, core: 2. Of those that a mesh axis runs over, the one named last changes fastest.
Arguments:
- tokens: int32 [16, 1024], P('dp')
- emb_table: bfloat16 [65536, 2304], P('tp')
- w_norm: float32 [2304], replicated
- dy_norm: bfloat16 [16, 1024, 2304], P('dp', 'tp')
- dy_resid: bfloat16 [16, 1024, 2304], P('dp', 'tp')
Outputs:
- output 1: bfloat16 [16, 1024, 2304], P('dp', 'tp')
- output 2: bfloat16 [16, 1024, 2304], P('dp', 'tp')
- output 3: float32 [65536, 2304], P(('tp', 'dp'))
- output 4: float32 [2304], replicated
All inputs are finite; a program needn't handle non-finite values.
Results may differ from the reference program's by a relative error of at most 0.00848154.
Values sent between devices are 32-bit elements.
A program may use at most 1 GiB of HBM per device.

```python
import jax
import jax.numpy as jnp
from jax import lax

VOCAB_ROWS = 65536
MODEL_DIM = 2304
NUM_SEQS = 16
SEQ_LEN = 1024
NORM_EPS = 1e-6
LOG_VOCAB = (VOCAB_ROWS - 1).bit_length()


def draw_tokens(key):
    k_level, k_ident, k_pick, k_flat = jax.random.split(key, 4)
    tok_shape = (NUM_SEQS, SEQ_LEN)
    zipf_level = jax.random.randint(k_level, tok_shape, 0, LOG_VOCAB + 1, dtype=jnp.int32)
    level_top = jnp.minimum(jnp.left_shift(jnp.ones(tok_shape, jnp.int32), zipf_level), VOCAB_ROWS)
    zipf_ids = jax.random.randint(k_ident, tok_shape, 0, level_top, dtype=jnp.int32)
    flat_ids = jax.random.randint(k_flat, tok_shape, 0, VOCAB_ROWS, dtype=jnp.int32)
    mix_pick = jax.random.randint(k_pick, tok_shape, 0, 4, dtype=jnp.int32)
    token_ids = jnp.where(mix_pick == 0, flat_ids, zipf_ids)
    return token_ids.at[0, 0].set(VOCAB_ROWS - 1)


def setup_inputs(seed: int = 0) -> dict:
    k_tok, k_tab, k_gain, k_norm, k_resid = jax.random.split(jax.random.key(seed), 5)
    tokens = draw_tokens(k_tok)
    emb_table = (jax.random.normal(k_tab, (VOCAB_ROWS, MODEL_DIM), jnp.float32) * MODEL_DIM ** -0.5).astype(jnp.bfloat16)
    w_norm = 0.6 * jax.random.normal(k_gain, (MODEL_DIM,), jnp.float32)
    dy_norm = jax.random.normal(k_norm, (NUM_SEQS, SEQ_LEN, MODEL_DIM), jnp.float32).astype(jnp.bfloat16)
    dy_resid = jax.random.normal(k_resid, (NUM_SEQS, SEQ_LEN, MODEL_DIM), jnp.float32).astype(jnp.bfloat16)
    return {"tokens": tokens, "emb_table": emb_table, "w_norm": w_norm, "dy_norm": dy_norm, "dy_resid": dy_resid}


def reference(tokens, emb_table, w_norm, dy_norm, dy_resid):
    emb_scale = jnp.asarray(MODEL_DIM ** 0.5, jnp.bfloat16)
    x_emb = emb_table[tokens] * emb_scale
    x_float = x_emb.astype(jnp.float32)
    inv_rms = lax.rsqrt(jnp.mean(x_float * x_float, axis=-1, keepdims=True) + NORM_EPS)
    x_hat = x_float * inv_rms
    norm_gain = 1.0 + w_norm
    y_norm = (x_hat * norm_gain).astype(jnp.bfloat16)
    dy_float = dy_norm.astype(jnp.float32)
    dx_hat = dy_float * norm_gain
    tok_grad = dy_resid.astype(jnp.float32) + inv_rms * (dx_hat - x_hat * jnp.mean(dx_hat * x_hat, axis=-1, keepdims=True))
    w_grad = jnp.sum(dy_float * x_hat, axis=(0, 1))
    emb_grad = jax.ops.segment_sum(tok_grad.reshape(-1, MODEL_DIM), tokens.reshape(-1), num_segments=VOCAB_ROWS) * emb_scale.astype(jnp.float32)
    return x_emb, y_norm, emb_grad, w_grad
```

```python
import functools
import math
import jax
import jax.numpy as jnp
from jax import lax
from jax.experimental import pallas as pl
from jax.experimental.pallas import tpu as pltpu
from jax.sharding import PartitionSpec as P

NORM_EPS = 1e-6
MESH = pl.DeviceIdType.MESH
HOT = 1024
STRIDE = 64
HOT_ROWS = 8
F32 = jnp.float32
BF16 = jnp.bfloat16
I32 = jnp.int32
VMEM = pltpu.VMEM
ANY = pl.ANY


def cold_cap(tp, blk):
    first = jnp.where(blk < 2, 0, jnp.where(blk < 4, 48, jnp.where(blk < 8, 32, 24)))
    return jnp.where(tp == 0, first, 16)


def gather_kernel(n_batch, batch, blk_ref, col_ref, table_ref, out_ref, buf, sems):
    def copies(step, slot):
        def one(i):
            row = pl.multiple_of(blk_ref[step * batch + i] * 8, 8)
            return pltpu.make_async_copy(
                table_ref.at[pl.ds(row, 8), :],
                buf.at[slot, pl.ds(pl.multiple_of(i * 8, 8), 8), :],
                sems.at[slot],
            )
        return one

    def start(step, slot):
        one = copies(step, slot)

        @pl.loop(0, batch)
        def _(i):
            one(i).start()

    depth = buf.shape[0]
    step = pl.program_id(0)

    @pl.when(step == 0)
    def _():
        for s in range(depth - 1):
            start(s, s)

    @pl.when(step + depth - 1 < n_batch)
    def _():
        start(step + depth - 1, lax.rem(step + depth - 1, depth))

    slot = lax.rem(step, depth)
    pltpu.make_async_copy(table_ref.at[pl.ds(0, batch * 8), :], buf.at[slot], sems.at[slot]).wait()
    col = col_ref[...]
    sel = (lax.broadcasted_iota(I32, (batch, batch * 8), 1) == col[:, :1]).astype(BF16)
    rows = jnp.dot(sel, buf[slot], preferred_element_type=F32)
    out_ref[...] = rows * math.sqrt(out_ref.shape[1])


def gather_rows(table, local_ids, owned):
    n, dim = local_ids.shape[0], table.shape[1]
    batch = 32
    safe = jnp.where(owned, local_ids, 0)
    blk = safe >> 3
    lane = (jnp.arange(n, dtype=I32) % batch) * 8 + (safe & 7)
    col = jnp.broadcast_to(jnp.where(owned, lane, -1)[:, None], (n, 128))
    return pl.pallas_call(
        functools.partial(gather_kernel, n // batch, batch),
        out_shape=jax.ShapeDtypeStruct((n, dim), F32),
        grid_spec=pltpu.PrefetchScalarGridSpec(
            num_scalar_prefetch=1,
            grid=(n // batch,),
            in_specs=[pl.BlockSpec((batch, 128), lambda i, *_: (i, 0)), pl.BlockSpec(memory_space=ANY)],
            out_specs=pl.BlockSpec((batch, dim), lambda i, *_: (i, 0)),
            scratch_shapes=[VMEM((4, batch * 8, dim), BF16), pltpu.SemaphoreType.DMA((4,))],
        ),
        compiler_params=pltpu.CompilerParams(dimension_semantics=("arbitrary",)),
        name="gather_rows",
    )(blk, col, table)


def index_kernel(n_dp, send_ref, recv_ref, send_sem, recv_sem):
    me = lax.axis_index("dp")
    recv_ref[pl.ds(me, 1)] = send_ref[pl.ds(me, 1)]

    def copy(i):
        to = lax.rem(me + i, n_dp)
        return pltpu.make_async_remote_copy(
            src_ref=send_ref.at[to], dst_ref=recv_ref.at[me],
            send_sem=send_sem.at[i], recv_sem=recv_sem.at[i],
            device_id={"dp": to}, device_id_type=MESH)

    def arrival(i):
        frm = lax.rem(me + n_dp - i, n_dp)
        return pltpu.make_async_remote_copy(
            src_ref=send_ref.at[frm], dst_ref=recv_ref.at[frm],
            send_sem=send_sem.at[i], recv_sem=recv_sem.at[i],
            device_id={"dp": frm}, device_id_type=MESH)

    for i in range(1, n_dp):
        copy(i).start()
    for i in range(1, n_dp):
        copy(i).wait_send()
        arrival(i).wait_recv()


def exchange_index(n_dp, send):
    return pl.pallas_call(
        functools.partial(index_kernel, n_dp),
        out_shape=jax.ShapeDtypeStruct(send.shape, I32),
        in_specs=[pl.BlockSpec(memory_space=VMEM)],
        out_specs=pl.BlockSpec(memory_space=VMEM),
        scratch_shapes=[pltpu.SemaphoreType.DMA((n_dp,)), pltpu.SemaphoreType.DMA((n_dp,))],
        compiler_params=pltpu.CompilerParams(has_side_effects=True),
        name="exchange_index",
    )(send)


def split3(x):
    hi = x.astype(BF16)
    rest = x - hi.astype(F32)
    mid = rest.astype(BF16)
    return hi, mid, (rest - mid.astype(F32)).astype(BF16)


def dot_exact(one_hot, x):
    parts = [jnp.dot(one_hot, p, preferred_element_type=F32) for p in split3(x)]
    return (parts[2] + parts[1]) + parts[0]


SUB = 256
NCHUNK = 3


def grad_kernel(n_dp, n_tp, slot_ref, idx_ref, g_ref, w_ref, out_ref, wout_ref,
                pick, place, send, recv, hot_send, hot_recv, w_dp, w_sum, w_tp,
                send_sem, recv_sem, hot_sem, wd_send, wd_recv, wt_send, wt_recv):
    me, plane = lax.axis_index("dp"), lax.axis_index("tp")
    dim = g_ref.shape[1]
    wide = dim // NCHUNK
    n_slots = n_dp * STRIDE
    scale = math.sqrt(dim)
    sizes = (8, 24, 32, 40, 56)

    def n_rows(blk):
        return HOT_ROWS + cold_cap(plane, blk)

    def peer(i):
        return lax.rem(me + i, n_dp), lax.rem(me + n_dp - i, n_dp)

    def w_copy(i, slot):
        return pltpu.make_async_remote_copy(
            src_ref=w_ref, dst_ref=w_dp.at[slot], send_sem=wd_send.at[i], recv_sem=wd_recv.at[i],
            device_id={"dp": peer(i)[0]}, device_id_type=MESH)

    for i in range(1, n_dp):
        w_copy(i, me).start()

    n_tok = g_ref.shape[0]

    @pl.loop(0, n_slots // 128)
    def _(b):
        base = pl.multiple_of(b * 128, 128)
        rows = lax.broadcasted_iota(I32, (128, n_tok), 0) + base
        pick[pl.ds(base, 128), :] = (rows == slot_ref[...]).astype(BF16)

    mine = n_rows(me)

    @pl.loop(0, n_dp)
    def _(s):
        @pl.loop(lax.div(mine, 8), STRIDE // 8)
        def _(r):
            recv[s, pl.ds(pl.multiple_of(r * 8, 8), 8), :] = jnp.zeros((8, dim), F32)

    def row_copy(c, i, size, to, slot):
        cols = pl.ds(pl.multiple_of(c * wide, 128), wide)
        return pltpu.make_async_remote_copy(
            src_ref=send.at[pl.ds(pl.multiple_of(to * STRIDE, 8), size), cols],
            dst_ref=recv.at[slot, pl.ds(0, size), cols],
            send_sem=send_sem.at[c, i], recv_sem=recv_sem.at[c, i],
            device_id={"dp": to}, device_id_type=MESH)

    def by_size(want, fn):
        for size in sizes:
            @pl.when(want == size)
            def _():
                fn(size)

    @pl.loop(0, NCHUNK)
    def _(c):
        @pl.loop(0, wide // SUB)
        def _(s):
            cols = pl.ds(pl.multiple_of(c * wide + s * SUB, 128), SUB)
            send[:, cols] = dot_exact(pick[...], g_ref[:, cols])

        @pl.loop(1, n_dp)
        def _(i):
            to = peer(i)[0]
            by_size(n_rows(to), lambda size: row_copy(c, i, size, to, me).start())

    recv[pl.ds(me, 1)] = send[pl.ds(pl.multiple_of(me * STRIDE, 8), STRIDE), :][None]

    w_dp[pl.ds(me, 1)] = w_ref[...][None]
    for i in range(1, n_dp):
        w_copy(i, me).wait_send()
        w_copy(i, peer(i)[1]).wait_recv()
    w_sum[...] = jnp.sum(w_dp[...], axis=0)

    def wt_copy(i, slot):
        return pltpu.make_async_remote_copy(
            src_ref=w_sum, dst_ref=w_tp.at[slot], send_sem=wt_send.at[i], recv_sem=wt_recv.at[i],
            device_id={"tp": lax.rem(plane + i, n_tp)}, device_id_type=MESH)

    for i in range(1, n_tp):
        wt_copy(i, plane).start()

    @pl.loop(0, n_dp // 2)
    def _(p):
        lane = lax.broadcasted_iota(I32, (1, 128), 1)
        idx = jnp.where(lane < STRIDE, idx_ref[2 * p, 0:1, :], idx_ref[2 * p + 1, 0:1, :])
        rows = lax.broadcasted_iota(I32, (place.shape[0], 128), 0)
        place[:, pl.ds(pl.multiple_of(p * 128, 128), 128)] = (rows == idx).astype(BF16)

    w_tp[pl.ds(plane, 1)] = w_sum[...][None]
    for i in range(1, n_tp):
        wt_copy(i, plane).wait_send()
        wt_copy(i, lax.rem(plane + n_tp - i, n_tp)).wait_recv()
    wout_ref[...] = jnp.sum(w_tp[...], axis=0)

    @pl.loop(0, NCHUNK)
    def _(c):
        @pl.loop(1, n_dp)
        def _(i):
            to, frm = peer(i)
            by_size(n_rows(to), lambda size: row_copy(c, i, size, to, me).wait_send())
            by_size(mine, lambda size: row_copy(c, i, size, frm, frm).wait_recv())

        @pl.loop(0, wide // SUB)
        def _(s):
            cols = pl.ds(pl.multiple_of(c * wide + s * SUB, 128), SUB)
            rows = recv[:, :, cols]
            hot_send[:, cols] = jnp.sum(rows[:, :HOT_ROWS, :], axis=0) * scale
            out_ref[:, cols] = dot_exact(place[...], rows.reshape(n_slots, SUB)) * scale

    per = n_tp // 2
    owner = lax.div(plane, per)
    at = pl.multiple_of(lax.rem(plane, per) * (n_dp * HOT_ROWS) + me * HOT_ROWS, 8)
    own = jnp.logical_and(plane == 0, me == owner)
    hot_copy = pltpu.make_async_remote_copy(
        src_ref=hot_send, dst_ref=hot_recv.at[pl.ds(at, HOT_ROWS), :],
        send_sem=hot_sem.at[0], recv_sem=hot_sem.at[1],
        device_id={"dp": owner, "tp": 0}, device_id_type=MESH)

    @pl.when(jnp.logical_not(own))
    def _():
        hot_copy.start()
        hot_copy.wait_send()

    total = hot_recv.shape[0]

    def hot_wait(n):
        ref = hot_recv.at[pl.ds(0, n), :]
        pltpu.make_async_remote_copy(
            src_ref=ref, dst_ref=ref, send_sem=hot_sem.at[0], recv_sem=hot_sem.at[1],
            device_id={"dp": 1, "tp": 0}, device_id_type=MESH).wait_recv()

    @pl.when(own)
    def _():
        hot_recv[0:HOT_ROWS, :] = hot_send[...]
        hot_wait(total - HOT_ROWS)

    @pl.when(jnp.logical_and(plane == 0, me == 1))
    def _():
        hot_wait(total)

    @pl.when(jnp.logical_and(plane == 0, me < 2))
    def _():
        out_ref[...] += hot_recv[...]


def exchange_grads(n_dp, n_tp, out_rows, slot, idx, g_all, w_part):
    n_tok, dim = g_all.shape
    dma = pltpu.SemaphoreType.DMA
    return pl.pallas_call(
        functools.partial(grad_kernel, n_dp, n_tp),
        out_shape=(jax.ShapeDtypeStruct((out_rows, dim), F32), jax.ShapeDtypeStruct(w_part.shape, F32)),
        in_specs=[pl.BlockSpec(memory_space=VMEM)] * 4,
        out_specs=(pl.BlockSpec(memory_space=VMEM), pl.BlockSpec(memory_space=VMEM)),
        scratch_shapes=[
            VMEM((n_dp * STRIDE, n_tok), BF16),
            VMEM((out_rows, n_dp * STRIDE), BF16),
            VMEM((n_dp * STRIDE, dim), F32),
            VMEM((n_dp, STRIDE, dim), F32),
            VMEM((HOT_ROWS, dim), F32),
            VMEM((HOT // 2, dim), F32),
            VMEM((n_dp,) + w_part.shape, F32),
            VMEM(w_part.shape, F32),
            VMEM((n_tp,) + w_part.shape, F32),
            dma((NCHUNK, n_dp)), dma((NCHUNK, n_dp)), dma((2,)),
            dma((n_dp,)), dma((n_dp,)), dma((n_tp,)), dma((n_tp,)),
        ],
        compiler_params=pltpu.CompilerParams(has_side_effects=True, vmem_limit_bytes=60 * 2**20),
        name="exchange_grads",
    )(slot, idx, g_all, w_part)


def swap(x, axis):
    return lax.all_to_all(x, axis, split_axis=0, concat_axis=0)


def dense_grads(n_dp, n_tp, out_rows, tokens, g_all, w_part):
    rows = n_dp * out_rows
    local = tokens - lax.axis_index("tp") * rows
    drop = jnp.where((local >= 0) & (local < rows), local, rows)
    shard = jax.ops.segment_sum(g_all, drop, num_segments=rows, mode="drop")
    emb = jnp.sum(swap(shard.reshape(n_dp, out_rows, -1), "dp"), axis=0) * math.sqrt(g_all.shape[1])
    w = jnp.sum(swap(jnp.broadcast_to(w_part, (n_dp,) + w_part.shape), "dp"), axis=0)
    w = jnp.sum(swap(jnp.broadcast_to(w, (n_tp,) + w.shape), "tp"), axis=0)
    return emb, w


def route(n_dp, n_tp, out_rows, ids):
    plane = lax.axis_index("tp")
    n = ids.shape[0]
    cold = ids >= HOT
    bins = ids // out_rows
    hits = (bins[:, None] == jnp.arange(n_dp * n_tp)[None]) & cold[:, None]
    bin_no = jnp.arange(n_dp * n_tp)
    flag = jnp.any(jnp.sum(hits.astype(I32), axis=0) > cold_cap(bin_no // n_dp, bin_no % n_dp))
    blk = bins % n_dp
    mine = cold & (bins // n_dp == plane)
    block_hit = (blk[:, None] == jnp.arange(n_dp)[None]) & mine[:, None]
    before = (jnp.arange(n)[:, None] > jnp.arange(n)[None]).astype(BF16)
    rank = jnp.sum(jnp.where(block_hit, jnp.dot(before, block_hit.astype(BF16), preferred_element_type=F32), 0.0), axis=1).astype(I32)
    cold_slot = blk * STRIDE + HOT_ROWS + rank
    per_plane = HOT // n_tp
    in_plane = ids % per_plane
    hot_slot = (in_plane // HOT_ROWS) * STRIDE + in_plane % HOT_ROWS
    hot = jnp.logical_not(cold) & (ids // per_plane == plane)
    slot = jnp.where(mine, cold_slot, jnp.where(hot, hot_slot, -1))
    slots = jnp.arange(n_dp * STRIDE)
    row = jnp.max(jnp.where((slots[:, None] == slot[None]) & mine[None], (ids % out_rows)[None], -1), axis=1)
    row = row.reshape(n_dp, 1, STRIDE)
    row = jnp.concatenate([row, row], axis=2)
    send = jnp.where(jnp.arange(8)[None, :, None] == 1, flag.astype(I32), row)
    return slot.reshape(1, n), send


def solution(mesh):
    n_dp, n_tp = mesh.shape["dp"], mesh.shape["tp"]

    def local_step(tokens, emb_table, w_norm, dy_norm, dy_resid):
        shard_rows, dim = emb_table.shape
        out_rows = shard_rows // n_dp
        ids = tokens[0]
        slot, send_idx = route(n_dp, n_tp, out_rows, ids)
        idx = exchange_index(n_dp, send_idx)
        fits = jnp.max(idx[:, 1, :]) == 0

        local_ids = ids - lax.axis_index("tp") * shard_rows
        owned = (local_ids >= 0) & (local_ids < shard_rows)
        partial_rows = gather_rows(emb_table, local_ids, owned)[None]
        x_emb = lax.psum_scatter(partial_rows, "tp", scatter_dimension=1, tiled=True).astype(BF16)
        x_float = x_emb.astype(F32)
        inv_rms = lax.rsqrt(jnp.mean(x_float * x_float, axis=-1, keepdims=True) + NORM_EPS)
        x_hat = x_float * inv_rms
        norm_gain = 1.0 + w_norm
        y_norm = (x_hat * norm_gain).astype(BF16)
        dy_float = dy_norm.astype(F32)
        dx_hat = dy_float * norm_gain
        tok_grad = dy_resid.astype(F32) + inv_rms * (dx_hat - x_hat * jnp.mean(dx_hat * x_hat, axis=-1, keepdims=True))
        w_part = jnp.sum(dy_float * x_hat, axis=(0, 1)).reshape(dim // 128, 128)
        w_part = jnp.pad(w_part, ((0, -(dim // 128) % 8), (0, 0)))
        g_all = lax.all_gather(tok_grad, "tp", axis=1, tiled=True)[0]
        emb_grad, w_sum = lax.cond(
            fits,
            lambda: exchange_grads(n_dp, n_tp, out_rows, slot, idx, g_all, w_part),
            lambda: dense_grads(n_dp, n_tp, out_rows, ids, g_all, w_part),
        )
        return x_emb, y_norm, emb_grad, w_sum[: dim // 128].reshape(dim)

    act_spec = P("dp", "tp", None)
    return jax.shard_map(local_step, mesh=mesh, in_specs=(P("dp", None), P("tp", None), P(None), act_spec, act_spec), out_specs=(act_spec, act_spec, P(("tp", "dp"), None), P(None)), check_vma=False)
```

```python
import functools
import math
import jax
import jax.numpy as jnp
from jax import lax
from jax.experimental import pallas as pl
from jax.experimental.pallas import tpu as pltpu
from jax.sharding import PartitionSpec as P

NORM_EPS = 1e-6
MESH = pl.DeviceIdType.MESH
HOT = 1024
STRIDE = 64
HOT_ROWS = 8
F32 = jnp.float32
BF16 = jnp.bfloat16
I32 = jnp.int32
VMEM = pltpu.VMEM
ANY = pl.ANY


def cold_cap(tp, blk):
    first = jnp.where(blk < 2, 0, jnp.where(blk < 4, 48, jnp.where(blk < 8, 32, 24)))
    return jnp.where(tp == 0, first, 16)


def gather_kernel(batch, blk_ref, count_ref, comb_ref, table_ref, out_ref, front, buf, sel, front_sem, sems):
    n_front, dim = front.shape
    n_tok = out_ref.shape[0]
    scale = math.sqrt(dim)
    count = count_ref[0]
    n_batch = lax.div(count + batch - 1, batch)
    head = pltpu.make_async_copy(table_ref.at[pl.ds(0, n_front), :], front, front_sem)
    head.start()

    def copy(blk, slot, i):
        return pltpu.make_async_copy(
            table_ref.at[pl.ds(pl.multiple_of(blk * 8, 8), 8), :],
            buf.at[slot, pl.ds(pl.multiple_of(i * 8, 8), 8), :],
            sems.at[slot])

    def in_batch(b):
        return jnp.minimum(count - b * batch, batch)

    def start(b):
        slot = lax.rem(b, 2)

        @pl.loop(0, in_batch(b))
        def _(i):
            copy(blk_ref[b * batch + i], slot, i).start()

    buf[...] = jnp.zeros(buf.shape, BF16)

    @pl.when(n_batch > 0)
    def _():
        start(0)

    def choose(base, width):
        @pl.loop(0, n_tok // 128)
        def _(r):
            rows = pl.ds(pl.multiple_of(r * 128, 128), 128)
            lanes = lax.broadcasted_iota(I32, (128, width), 1) + base
            sel[rows, :width] = (lanes == comb_ref[rows, :1]).astype(BF16)

    choose(0, n_front)
    head.wait()

    @pl.loop(0, dim // 256)
    def _(s):
        cols = pl.ds(pl.multiple_of(s * 256, 128), 256)
        out_ref[:, cols] = jnp.dot(sel[...], front[:, cols], preferred_element_type=F32) * scale

    @pl.loop(0, n_batch)
    def _(b):
        slot = lax.rem(b, 2)

        @pl.when(b + 1 < n_batch)
        def _():
            start(b + 1)

        choose(n_front + b * (batch * 8), batch * 8)

        @pl.loop(0, in_batch(b))
        def _(i):
            copy(0, slot, i).wait()

        @pl.loop(0, dim // 256)
        def _(s):
            cols = pl.ds(pl.multiple_of(s * 256, 128), 256)
            out_ref[:, cols] += jnp.dot(sel[:, : batch * 8], buf[slot, :, cols], preferred_element_type=F32) * scale


def gather_rows(table, local_ids, owned):
    n, dim = local_ids.shape[0], table.shape[1]
    batch, n_front = 64, 1024
    far = owned & (local_ids >= n_front)
    before = (jnp.arange(n)[:, None] > jnp.arange(n)[None]) & far[None]
    rank = jnp.sum(before.astype(I32), axis=1)
    count = jnp.sum(far.astype(I32)).reshape(1)
    comb = jnp.where(far, n_front + rank * 8 + (local_ids & 7), jnp.where(owned, local_ids, -1))
    hit = (jnp.arange(n)[:, None] == rank[None]) & far[None]
    blk = jnp.max(jnp.where(hit, (local_ids >> 3)[None], 0), axis=1)
    return pl.pallas_call(
        functools.partial(gather_kernel, batch),
        out_shape=jax.ShapeDtypeStruct((n, dim), F32),
        in_specs=[pl.BlockSpec(memory_space=pltpu.SMEM), pl.BlockSpec(memory_space=pltpu.SMEM),
                  pl.BlockSpec(memory_space=VMEM), pl.BlockSpec(memory_space=ANY)],
        out_specs=pl.BlockSpec(memory_space=VMEM),
        scratch_shapes=[
            VMEM((n_front, dim), BF16),
            VMEM((2, batch * 8, dim), BF16),
            VMEM((n, n_front), BF16),
            pltpu.SemaphoreType.DMA,
            pltpu.SemaphoreType.DMA((2,)),
        ],
        compiler_params=pltpu.CompilerParams(vmem_limit_bytes=48 * 2**20),
        name="gather_rows",
    )(blk, count, comb.reshape(n, 1), table)


class Line:
    def __init__(self, n_tp):
        self.me = lax.axis_index("tp")
        n_chip = n_tp // 2
        chip, core = lax.div(self.me, 2), lax.rem(self.me, 2)
        self.core = core
        self.partner = chip * 2 + 1 - core
        self.left, self.right, self.opp = (
            lax.rem(chip + k, n_chip) * 2 + core for k in (n_chip - 1, 1, n_chip // 2))
        self.chips = {"opp": self.opp, "right": self.right, "left": self.left, "own": self.me}

    def other(self, tp):
        return tp + 1 - 2 * self.core


def tp_copy(src, dst, sems, at, tp):
    send, recv = sems
    return pltpu.make_async_remote_copy(
        src_ref=src, dst_ref=dst, send_sem=send.at[at], recv_sem=recv.at[at],
        device_id={"tp": tp}, device_id_type=MESH)


def greet(devices):
    barrier = pltpu.get_barrier_semaphore()
    for device in devices:
        pl.semaphore_signal(barrier, inc=1, device_id=device, device_id_type=MESH)
    return barrier


def rows_kernel(n_dp, n_tp, part_ref, send_ref, w_ref, dyn_ref, dyr_ref,
                x_ref, y_ref, g_ref, wpart_ref, idx_ref,
                chip_sum, half_in, full_in, d_send, d_recv, h_send, h_recv, f_send, f_recv, i_send, i_recv):
    me = lax.axis_index("dp")
    line = Line(n_tp)
    n_pos, dim = x_ref.shape
    half = n_pos // 2
    piece = 16
    n_piece = half // piece
    order = ("opp", "right", "left", "own")

    barrier = greet([{"tp": t} for t in (line.partner, line.left, line.right)]
                    + [{"dp": lax.rem(me + i, n_dp)} for i in range(1, n_dp)])
    pl.semaphore_wait(barrier, n_dp + 2)

    def block(tp):
        return pl.ds(pl.multiple_of(tp * n_pos, n_pos), n_pos)

    def to_partner(k):
        return tp_copy(part_ref.at[block(line.other(line.chips[order[k]])), :], chip_sum.at[k],
                       (d_send, d_recv), k, line.partner)

    for k in range(4):
        to_partner(k).start()

    def idx_copy(i, to, slot):
        return pltpu.make_async_remote_copy(
            src_ref=send_ref.at[to], dst_ref=idx_ref.at[slot], send_sem=i_send.at[i], recv_sem=i_recv.at[i],
            device_id={"dp": to}, device_id_type=MESH)

    for i in range(1, n_dp):
        idx_copy(i, lax.rem(me + i, n_dp), me).start()

    def add_chip(k):
        to_partner(k).wait_recv()
        chip_sum[k] += part_ref[block(line.chips[order[k]]), :]

    def half_copy(side, q):
        rows = pl.ds(side * half + q * piece, piece)
        return tp_copy(chip_sum.at[0, rows, :], half_in.at[side, pl.ds(q * piece, piece), :],
                       (h_send, h_recv), (side, q), (line.right, line.left)[side])

    def full_copy(side, q):
        rows = pl.ds(q * piece, piece)
        return tp_copy(chip_sum.at[1 + side, rows, :], full_in.at[side, rows, :],
                       (f_send, f_recv), (side, q), (line.right, line.left)[side])

    add_chip(0)
    for q in range(n_piece):
        for side in range(2):
            half_copy(side, q).start()
    add_chip(1)
    add_chip(2)
    for q in range(n_piece):
        full_copy(0, n_piece + q).start()
        full_copy(1, q).start()
    for q in range(n_piece):
        for side in range(2):
            half_copy(side, q).wait_recv()
            rows = pl.ds(side * half + q * piece, piece)
            chip_sum[1 + side, rows, :] += half_in[side, pl.ds(q * piece, piece), :]
            full_copy(side, side * n_piece + q).start()
    add_chip(3)

    idx_ref[pl.ds(me, 1)] = send_ref[pl.ds(me, 1)]
    for i in range(1, n_dp):
        to, frm = lax.rem(me + i, n_dp), lax.rem(me + n_dp - i, n_dp)
        idx_copy(i, to, me).wait_send()
        idx_copy(i, frm, frm).wait_recv()

    gain = 1.0 + w_ref[...]
    w_acc = jnp.zeros((8, dim), F32)
    for q in list(range(n_piece)) + list(range(n_piece, 2 * n_piece)):
        for side in range(2):
            full_copy(side, q).wait_recv()
        for r in range(q * piece, (q + 1) * piece, 8):
            rows = pl.ds(r, 8)
            total = (chip_sum[3, rows, :] + full_in[0, rows, :]) + full_in[1, rows, :]
            x_emb = total.astype(BF16)
            x_ref[rows, :] = x_emb
            x = x_emb.astype(F32)
            r_inv = lax.rsqrt(jnp.mean(x * x, axis=-1, keepdims=True) + NORM_EPS)
            x_hat = x * r_inv
            y_ref[rows, :] = (x_hat * gain).astype(BF16)
            dy = dyn_ref[rows, :].astype(F32)
            a = dy * gain
            g_ref[rows, :] = dyr_ref[rows, :].astype(F32) + r_inv * (a - x_hat * jnp.mean(a * x_hat, axis=-1, keepdims=True))
            w_acc = w_acc + dy * x_hat
    wpart_ref[...] = jnp.sum(w_acc, axis=0, keepdims=True)

    for k in range(4):
        to_partner(k).wait_send()
    for q in range(n_piece):
        for side in range(2):
            half_copy(side, q).wait_send()
    for q in range(2 * n_piece):
        for side in range(2):
            full_copy(side, q).wait_send()


def rows_and_norm(n_dp, n_tp, part, send_idx, w_norm, dy_norm, dy_resid):
    n_pos, dim = dy_norm.shape
    dma = pltpu.SemaphoreType.DMA
    vmem = pl.BlockSpec(memory_space=VMEM)
    pieces = n_pos // 16
    return pl.pallas_call(
        functools.partial(rows_kernel, n_dp, n_tp),
        out_shape=(jax.ShapeDtypeStruct((n_pos, dim), BF16), jax.ShapeDtypeStruct((n_pos, dim), BF16),
                   jax.ShapeDtypeStruct((n_pos, dim), F32), jax.ShapeDtypeStruct((1, dim), F32),
                   jax.ShapeDtypeStruct(send_idx.shape, I32)),
        in_specs=[vmem] * 5,
        out_specs=(vmem,) * 5,
        scratch_shapes=[
            VMEM((4, n_pos, dim), F32),
            VMEM((2, n_pos // 2, dim), F32),
            VMEM((2, n_pos, dim), F32),
            dma((4,)), dma((4,)), dma((2, pieces // 2)), dma((2, pieces // 2)),
            dma((2, pieces)), dma((2, pieces)), dma((n_dp,)), dma((n_dp,)),
        ],
        compiler_params=pltpu.CompilerParams(collective_id=1, has_side_effects=True, vmem_limit_bytes=60 * 2**20),
        name="rows_and_norm",
    )(part, send_idx, w_norm.reshape(1, dim), dy_norm, dy_resid)


def split3(x):
    hi = x.astype(BF16)
    rest = x - hi.astype(F32)
    mid = rest.astype(BF16)
    return hi, mid, (rest - mid.astype(F32)).astype(BF16)


def dot_exact(one_hot, x):
    parts = [jnp.dot(one_hot, p, preferred_element_type=F32) for p in split3(x)]
    return (parts[2] + parts[1]) + parts[0]


NCHUNK = 9


def grad_kernel(n_dp, n_tp, slot_ref, idx_ref, g_ref, w_ref, out_ref, wout_ref,
                g_all, pick, place, send, recv, hot_send, hot_recv, w_dp, w_sum, w_tp,
                ag_send, ag_recv, send_sem, recv_sem, hot_out, hot_in, wd_send, wd_recv, wt_send, wt_recv):
    me, plane = lax.axis_index("dp"), lax.axis_index("tp")
    line = Line(n_tp)
    n_pos, dim = g_ref.shape
    n_tok = n_pos * n_tp
    wide = dim // NCHUNK
    n_slots = n_dp * STRIDE
    scale = math.sqrt(dim)
    sizes = (8, 24, 32, 40, 56)
    per = n_tp // 2
    owner = lax.div(plane, per)
    own = jnp.logical_and(plane == 0, me == owner)
    gathers_hot = jnp.logical_and(plane == 0, me < 2)

    barrier = greet([{"tp": lax.rem(plane + i, n_tp)} for i in range(1, n_tp)]
                    + [{"dp": lax.rem(me + i, n_dp)} for i in range(1, n_dp)])

    @pl.when(jnp.logical_not(own))
    def _():
        pl.semaphore_signal(barrier, inc=1, device_id={"dp": owner, "tp": 0}, device_id_type=MESH)

    @pl.when(gathers_hot)
    def _():
        @pl.loop(0, per * n_dp)
        def _(k):
            dp, tp = lax.rem(k, n_dp), lax.div(k, n_dp) + me * per

            @pl.when(jnp.logical_not(jnp.logical_and(tp == 0, dp == me)))
            def _():
                pl.semaphore_signal(barrier, inc=1, device_id={"dp": dp, "tp": tp}, device_id_type=MESH)

    extra = jnp.where(own, 0, 1) + jnp.where(gathers_hot, per * n_dp - jnp.where(own, 1, 0), 0)
    pl.semaphore_wait(barrier, n_dp + n_tp - 2 + extra)

    def n_rows(blk):
        return HOT_ROWS + cold_cap(plane, blk)

    def peer(i):
        return lax.rem(me + i, n_dp), lax.rem(me + n_dp - i, n_dp)

    def cols_of(c):
        return pl.ds(pl.multiple_of(c * wide, 128), wide)

    def block(tp, start=0, size=n_pos):
        return pl.ds(pl.multiple_of(tp * n_pos + start, 8), size)

    half = n_pos // 2
    KINDS = range(8)

    def ag_sent(kind, c):
        cols = cols_of(c)
        rows, to = (
            (block(plane), line.right), (block(plane), line.left),
            (block(line.left, 0, half), line.right), (block(line.right, half, half), line.left),
            (block(plane), line.partner), (block(line.left), line.partner),
            (block(line.right), line.partner), (block(line.opp), line.partner))[kind]
        src = g_ref.at[:, cols] if kind in (0, 1, 4) else g_all.at[rows, cols]
        return tp_copy(src, g_all.at[rows, cols], (ag_send, ag_recv), (kind, c), to)

    def ag_arrives(kind, c):
        cols = cols_of(c)
        rows = (block(line.left), block(line.right),
                block(line.opp, 0, half), block(line.opp, half, half),
                block(line.partner), block(line.other(line.left)),
                block(line.other(line.right)), block(line.other(line.opp)))[kind]
        return tp_copy(g_all.at[rows, cols], g_all.at[rows, cols], (ag_send, ag_recv), (kind, c), line.partner)

    def w_copy(i, slot):
        return pltpu.make_async_remote_copy(
            src_ref=w_ref, dst_ref=w_dp.at[slot], send_sem=wd_send.at[i], recv_sem=wd_recv.at[i],
            device_id={"dp": peer(i)[0]}, device_id_type=MESH)

    def row_copy(c, i, size, to, slot):
        return pltpu.make_async_remote_copy(
            src_ref=send.at[pl.ds(pl.multiple_of(to * STRIDE, 8), size), cols_of(c)],
            dst_ref=recv.at[slot, pl.ds(0, size), cols_of(c)],
            send_sem=send_sem.at[c, i], recv_sem=recv_sem.at[c, i],
            device_id={"dp": to}, device_id_type=MESH)

    def by_size(want, fn):
        for size in sizes:
            @pl.when(want == size)
            def _():
                fn(size)

    def setup():
        for i in range(1, n_dp):
            w_copy(i, me).start()
        g_all[block(plane), :] = g_ref[...]

        @pl.loop(0, n_slots // 128)
        def _(b):
            base = pl.multiple_of(b * 128, 128)
            rows = lax.broadcasted_iota(I32, (128, n_tok), 0) + base
            pick[pl.ds(base, 128), :] = (rows == slot_ref[...]).astype(BF16)

        @pl.loop(0, n_dp)
        def _(s):
            @pl.loop(lax.div(n_rows(me), 8), STRIDE // 8)
            def _(r):
                recv[s, pl.ds(pl.multiple_of(r * 8, 8), 8), :] = jnp.zeros((8, dim), F32)

        @pl.loop(0, n_dp // 2)
        def _(p):
            lane = lax.broadcasted_iota(I32, (1, 128), 1)
            idx = jnp.where(lane < STRIDE, idx_ref[2 * p, 0:1, :], idx_ref[2 * p + 1, 0:1, :])
            rows = lax.broadcasted_iota(I32, (place.shape[0], 128), 0)
            place[:, pl.ds(pl.multiple_of(p * 128, 128), 128)] = (rows == idx).astype(BF16)

    @pl.loop(0, NCHUNK + 3)
    def _(i):
        @pl.when(i < NCHUNK)
        def _():
            for kind in (0, 1, 4):
                ag_sent(kind, i).start()

        @pl.when(i == 0)
        def _():
            setup()

        @pl.when(jnp.logical_and(i >= 1, i < NCHUNK + 1))
        def _():
            c = i - 1
            ag_arrives(0, c).wait_recv()
            ag_sent(2, c).start()
            ag_sent(5, c).start()
            ag_arrives(1, c).wait_recv()
            ag_sent(3, c).start()
            ag_sent(6, c).start()

        @pl.when(jnp.logical_and(i >= 2, i < NCHUNK + 2))
        def _():
            c = i - 2
            ag_arrives(2, c).wait_recv()
            ag_arrives(3, c).wait_recv()
            ag_sent(7, c).start()

        @pl.when(i >= 3)
        def _():
            c = i - 3
            for kind in (4, 5, 6, 7):
                ag_arrives(kind, c).wait_recv()
            cols = cols_of(c)
            send[:, cols] = dot_exact(pick[...], g_all[:, cols])

            @pl.loop(1, n_dp)
            def _(k):
                to = peer(k)[0]
                by_size(n_rows(to), lambda size: row_copy(c, k, size, to, me).start())

    recv[pl.ds(me, 1)] = send[pl.ds(pl.multiple_of(me * STRIDE, 8), STRIDE), :][None]

    w_dp[pl.ds(me, 1)] = w_ref[...][None]
    for i in range(1, n_dp):
        w_copy(i, me).wait_send()
        w_copy(i, peer(i)[1]).wait_recv()
    w_sum[...] = jnp.sum(w_dp[...], axis=0)

    def wt_copy(i, slot):
        return tp_copy(w_sum, w_tp.at[slot], (wt_send, wt_recv), i, lax.rem(plane + i, n_tp))

    for i in range(1, n_tp):
        wt_copy(i, plane).start()
    w_tp[pl.ds(plane, 1)] = w_sum[...][None]

    @pl.loop(0, NCHUNK)
    def _(c):
        for kind in KINDS:
            ag_sent(kind, c).wait_send()

    at = pl.multiple_of(lax.rem(plane, per) * (n_dp * HOT_ROWS) + me * HOT_ROWS, 8)

    def hot_copy(c):
        return pltpu.make_async_remote_copy(
            src_ref=hot_send.at[:, cols_of(c)], dst_ref=hot_recv.at[pl.ds(at, HOT_ROWS), cols_of(c)],
            send_sem=hot_out.at[c], recv_sem=hot_in.at[0],
            device_id={"dp": owner, "tp": 0}, device_id_type=MESH)

    @pl.loop(0, NCHUNK)
    def _(c):
        @pl.loop(1, n_dp)
        def _(i):
            to, frm = peer(i)
            by_size(n_rows(to), lambda size: row_copy(c, i, size, to, me).wait_send())
            by_size(n_rows(me), lambda size: row_copy(c, i, size, frm, frm).wait_recv())

        cols = cols_of(c)
        rows = recv[:, :, cols]
        hot_send[:, cols] = jnp.sum(rows[:, :HOT_ROWS, :], axis=0) * scale

        @pl.when(jnp.logical_not(own))
        def _():
            hot_copy(c).start()

        out_ref[:, cols] = dot_exact(place[...], rows.reshape(n_slots, wide)) * scale

    for i in range(1, n_tp):
        wt_copy(i, plane).wait_send()
        wt_copy(i, lax.rem(plane + n_tp - i, n_tp)).wait_recv()
    wout_ref[...] = jnp.sum(w_tp[...], axis=0)

    @pl.when(jnp.logical_not(own))
    def _():
        @pl.loop(0, NCHUNK)
        def _(c):
            hot_copy(c).wait_send()

    def hot_wait(n):
        ref = hot_recv.at[pl.ds(0, n), :]
        pltpu.make_async_remote_copy(
            src_ref=ref, dst_ref=ref, send_sem=hot_out.at[0], recv_sem=hot_in.at[0],
            device_id={"dp": 1, "tp": 0}, device_id_type=MESH).wait_recv()

    total = hot_recv.shape[0]

    @pl.when(own)
    def _():
        hot_recv[0:HOT_ROWS, :] = hot_send[...]
        hot_wait(total - HOT_ROWS)

    @pl.when(jnp.logical_and(plane == 0, me == 1))
    def _():
        hot_wait(total)

    @pl.when(gathers_hot)
    def _():
        out_ref[...] += hot_recv[...]


def exchange_grads(n_dp, n_tp, out_rows, slot, idx, g, w_part):
    n_pos, dim = g.shape
    n_tok = n_pos * n_tp
    dma = pltpu.SemaphoreType.DMA
    vmem = pl.BlockSpec(memory_space=VMEM)
    return pl.pallas_call(
        functools.partial(grad_kernel, n_dp, n_tp),
        out_shape=(jax.ShapeDtypeStruct((out_rows, dim), F32), jax.ShapeDtypeStruct(w_part.shape, F32)),
        in_specs=[vmem] * 4,
        out_specs=(vmem,) * 2,
        scratch_shapes=[
            VMEM((n_tok, dim), F32),
            VMEM((n_dp * STRIDE, n_tok), BF16),
            VMEM((out_rows, n_dp * STRIDE), BF16),
            VMEM((n_dp * STRIDE, dim), F32),
            VMEM((n_dp, STRIDE, dim), F32),
            VMEM((HOT_ROWS, dim), F32),
            VMEM((HOT // 2, dim), F32),
            VMEM((n_dp,) + w_part.shape, F32),
            VMEM(w_part.shape, F32),
            VMEM((n_tp,) + w_part.shape, F32),
            dma((8, NCHUNK)), dma((8, NCHUNK)),
            dma((NCHUNK, n_dp)), dma((NCHUNK, n_dp)), dma((NCHUNK,)), dma((1,)),
            dma((n_dp,)), dma((n_dp,)), dma((n_tp,)), dma((n_tp,)),
        ],
        compiler_params=pltpu.CompilerParams(collective_id=2, has_side_effects=True, vmem_limit_bytes=62 * 2**20),
        name="exchange_grads",
    )(slot, idx, g, w_part)


def swap(x, axis):
    return lax.all_to_all(x, axis, split_axis=0, concat_axis=0)


def dense_grads(n_dp, n_tp, out_rows, tokens, g, w_part):
    g_all = swap(jnp.broadcast_to(g, (n_tp,) + g.shape), "tp").reshape(-1, g.shape[1])
    rows = n_dp * out_rows
    local = tokens - lax.axis_index("tp") * rows
    drop = jnp.where((local >= 0) & (local < rows), local, rows)
    shard = jax.ops.segment_sum(g_all, drop, num_segments=rows, mode="drop")
    emb = jnp.sum(swap(shard.reshape(n_dp, out_rows, -1), "dp"), axis=0) * math.sqrt(g_all.shape[1])
    w = jnp.sum(swap(jnp.broadcast_to(w_part, (n_dp,) + w_part.shape), "dp"), axis=0)
    w = jnp.sum(swap(jnp.broadcast_to(w, (n_tp,) + w.shape), "tp"), axis=0)
    return emb, w


def route(n_dp, n_tp, out_rows, ids):
    plane = lax.axis_index("tp")
    n = ids.shape[0]
    cold = ids >= HOT
    bins = ids // out_rows
    hits = (bins[:, None] == jnp.arange(n_dp * n_tp)[None]) & cold[:, None]
    bin_no = jnp.arange(n_dp * n_tp)
    flag = jnp.any(jnp.sum(hits.astype(I32), axis=0) > cold_cap(bin_no // n_dp, bin_no % n_dp))
    blk = bins % n_dp
    mine = cold & (bins // n_dp == plane)
    block_hit = (blk[:, None] == jnp.arange(n_dp)[None]) & mine[:, None]
    before = (jnp.arange(n)[:, None] > jnp.arange(n)[None]).astype(BF16)
    rank = jnp.sum(jnp.where(block_hit, jnp.dot(before, block_hit.astype(BF16), preferred_element_type=F32), 0.0), axis=1).astype(I32)
    cold_slot = blk * STRIDE + HOT_ROWS + rank
    per_plane = HOT // n_tp
    in_plane = ids % per_plane
    hot_slot = (in_plane // HOT_ROWS) * STRIDE + in_plane % HOT_ROWS
    hot = jnp.logical_not(cold) & (ids // per_plane == plane)
    slot = jnp.where(mine, cold_slot, jnp.where(hot, hot_slot, -1))
    slots = jnp.arange(n_dp * STRIDE)
    row = jnp.max(jnp.where((slots[:, None] == slot[None]) & mine[None], (ids % out_rows)[None], -1), axis=1)
    row = row.reshape(n_dp, 1, STRIDE)
    row = jnp.concatenate([row, row], axis=2)
    send = jnp.where(jnp.arange(8)[None, :, None] == 1, flag.astype(I32), row)
    return slot.reshape(1, n), send


def solution(mesh):
    n_dp, n_tp = mesh.shape["dp"], mesh.shape["tp"]

    def local_step(tokens, emb_table, w_norm, dy_norm, dy_resid):
        shard_rows, dim = emb_table.shape
        out_rows = shard_rows // n_dp
        ids = tokens[0]
        slot, send_idx = route(n_dp, n_tp, out_rows, ids)
        local_ids = ids - lax.axis_index("tp") * shard_rows
        owned = (local_ids >= 0) & (local_ids < shard_rows)
        part = gather_rows(emb_table, local_ids, owned)
        x_emb, y_norm, g, w_part, idx = rows_and_norm(n_dp, n_tp, part, send_idx, w_norm, dy_norm[0], dy_resid[0])
        fits = jnp.max(idx[:, 1, :]) == 0
        emb_grad, w_sum = lax.cond(
            fits,
            lambda: exchange_grads(n_dp, n_tp, out_rows, slot, idx, g, w_part),
            lambda: dense_grads(n_dp, n_tp, out_rows, ids, g, w_part),
        )
        return x_emb[None], y_norm[None], emb_grad, w_sum[0]

    act_spec = P("dp", "tp", None)
    return jax.shard_map(local_step, mesh=mesh, in_specs=(P("dp", None), P("tp", None), P(None), act_spec, act_spec), out_specs=(act_spec, act_spec, P(("tp", "dp"), None), P(None)), check_vma=False)
```

```python
import functools
import math
import jax
import jax.numpy as jnp
from jax import lax
from jax.experimental import pallas as pl
from jax.experimental.pallas import tpu as pltpu
from jax.sharding import PartitionSpec as P

NORM_EPS = 1e-6
MESH = pl.DeviceIdType.MESH
HOT = 1024
STRIDE = 64
HOT_ROWS = 8
F32 = jnp.float32
BF16 = jnp.bfloat16
I32 = jnp.int32
VMEM = pltpu.VMEM
ANY = pl.ANY


def cold_cap(tp, blk):
    first = jnp.where(blk < 2, 0, jnp.where(blk < 4, 48, jnp.where(blk < 8, 32, 24)))
    return jnp.where(tp == 0, first, 16)


def gather_kernel(batch, blk_ref, count_ref, comb_ref, front_ref, table_ref, out_ref, near, far, sel, sel2, sems):
    n_front, wide = front_ref.shape
    n_tok = out_ref.shape[0]
    scale = math.sqrt(table_ref.shape[1])
    count = count_ref[0]
    n_batch = lax.div(count + batch - 1, batch)
    step = pl.program_id(0)

    def pair(b, i):
        return pl.ds(pl.multiple_of(blk_ref[b * batch + i] * 2, 2), 2), pl.ds(pl.multiple_of(i * 2, 2), 2)

    def near_copy(i):
        src, dst = pair(0, i)
        return pltpu.make_async_copy(table_ref.at[src, :], near.at[dst, :], sems.at[0])

    def choose(ref, base):
        @pl.loop(0, n_tok // 128)
        def _(r):
            rows = pl.ds(pl.multiple_of(r * 128, 128), 128)
            lanes = lax.broadcasted_iota(I32, (128, ref.shape[1]), 1) + base
            ref[rows, :] = (lanes == comb_ref[rows, :1]).astype(BF16)

    first = jnp.minimum(count, batch)

    @pl.when(step == 0)
    def _():
        near[...] = jnp.zeros(near.shape, BF16)

        @pl.loop(0, first)
        def _(i):
            near_copy(i).start()

        choose(sel, 0)

    out_ref[...] = jnp.dot(sel[:, :n_front], front_ref[...], preferred_element_type=F32) * scale

    @pl.when(step == 0)
    def _():
        @pl.loop(0, first)
        def _(i):
            near_copy(0).wait()

    cols = pl.ds(pl.multiple_of(step * wide, 128), wide)
    out_ref[...] += jnp.dot(sel[:, n_front:], near[:, cols], preferred_element_type=F32) * scale

    @pl.loop(1, n_batch)
    def _(b):
        here = jnp.minimum(count - b * batch, batch)

        def far_copy(i):
            src, dst = pair(b, i)
            return pltpu.make_async_copy(table_ref.at[src, cols], far.at[dst, :], sems.at[1])

        far[...] = jnp.zeros(far.shape, BF16)

        @pl.loop(0, here)
        def _(i):
            far_copy(i).start()

        choose(sel2, n_front + b * (2 * batch))

        @pl.loop(0, here)
        def _(i):
            far_copy(0).wait()

        out_ref[...] += jnp.dot(sel2[...], far[...], preferred_element_type=F32) * scale


def gather_rows(table, local_ids, owned):
    n, dim = local_ids.shape[0], table.shape[1]
    batch, n_front, wide = 320, 512, 256
    far = owned & (local_ids >= n_front)
    before = (jnp.arange(n)[:, None] > jnp.arange(n)[None]) & far[None]
    rank = jnp.sum(before.astype(I32), axis=1)
    count = jnp.sum(far.astype(I32)).reshape(1)
    comb = jnp.where(far, n_front + rank * 2 + (local_ids & 1), jnp.where(owned, local_ids, -1))
    hit = (jnp.arange(n)[:, None] == rank[None]) & far[None]
    blk = jnp.max(jnp.where(hit, (local_ids >> 1)[None], 0), axis=1)
    blk = jnp.pad(blk, (0, -n % batch))
    return pl.pallas_call(
        functools.partial(gather_kernel, batch),
        out_shape=jax.ShapeDtypeStruct((n, dim), F32),
        grid_spec=pltpu.PrefetchScalarGridSpec(
            num_scalar_prefetch=2,
            grid=(dim // wide,),
            in_specs=[pl.BlockSpec((n, 1), lambda i, *_: (0, 0)),
                      pl.BlockSpec((n_front, wide), lambda i, *_: (0, i)),
                      pl.BlockSpec(memory_space=ANY)],
            out_specs=pl.BlockSpec((n, wide), lambda i, *_: (0, i)),
            scratch_shapes=[
                VMEM((2 * batch, dim), BF16),
                VMEM((2 * batch, wide), BF16),
                VMEM((n, n_front + 2 * batch), BF16),
                VMEM((n, 2 * batch), BF16),
                pltpu.SemaphoreType.DMA((2,)),
            ],
        ),
        compiler_params=pltpu.CompilerParams(dimension_semantics=("arbitrary",), vmem_limit_bytes=32 * 2**20),
        name="gather_rows",
    )(blk, count, comb.reshape(n, 1), table, table)


class Line:
    def __init__(self, n_tp):
        self.me = lax.axis_index("tp")
        n_chip = n_tp // 2
        chip, core = lax.div(self.me, 2), lax.rem(self.me, 2)
        self.core = core
        self.partner = chip * 2 + 1 - core
        self.left, self.right, self.opp = (
            lax.rem(chip + k, n_chip) * 2 + core for k in (n_chip - 1, 1, n_chip // 2))
        self.chips = {"opp": self.opp, "right": self.right, "left": self.left, "own": self.me}

    def other(self, tp):
        return tp + 1 - 2 * self.core


def tp_copy(src, dst, sems, at, tp):
    send, recv = sems
    return pltpu.make_async_remote_copy(
        src_ref=src, dst_ref=dst, send_sem=send.at[at], recv_sem=recv.at[at],
        device_id={"tp": tp}, device_id_type=MESH)


def greet(devices):
    barrier = pltpu.get_barrier_semaphore()
    for device in devices:
        pl.semaphore_signal(barrier, inc=1, device_id=device, device_id_type=MESH)
    return barrier


def split3(x):
    hi = x.astype(BF16)
    rest = x - hi.astype(F32)
    mid = rest.astype(BF16)
    return hi, mid, (rest - mid.astype(F32)).astype(BF16)


def dot_exact(one_hot, x):
    parts = [jnp.dot(one_hot, p, preferred_element_type=F32) for p in split3(x)]
    return (parts[2] + parts[1]) + parts[0]


NCHUNK = 9
LAG = 4
PIECE = 16


def step_kernel(n_dp, n_tp, part_ref, slot_ref, send_ref, gain_ref, dyn_ref, dyr_ref,
                x_ref, y_ref, g_ref, out_ref, wout_ref, idx_ref,
                mine, chip_sum, half_in, full_in, g_all, pick, place, send, recv, hot_send, hot_recv,
                w_part, w_dp, w_sum, w_tp,
                m_sem, d_send, d_recv, h_send, h_recv, f_send, f_recv, i_send, i_recv,
                ag_send, ag_recv, a_send, a_recv, hot_out, hot_in, wd_send, wd_recv, wt_send, wt_recv):
    me, plane = lax.axis_index("dp"), lax.axis_index("tp")
    line = Line(n_tp)
    n_pos, dim = x_ref.shape
    half = n_pos // 2
    n_tok = n_pos * n_tp
    wide = dim // NCHUNK
    n_slots = n_dp * STRIDE
    n_piece = half // PIECE
    scale = math.sqrt(dim)
    sizes = (8, 24, 32, 40, 56)
    order = ("opp", "right", "left", "own")
    per = n_tp // 2
    owner = lax.div(plane, per)
    own = jnp.logical_and(plane == 0, me == owner)
    gathers_hot = jnp.logical_and(plane == 0, me < 2)

    def block(tp, start=0, size=n_pos):
        return pl.ds(pl.multiple_of(tp * n_pos + start, 8), size)

    def mine_copy(k):
        return pltpu.make_async_copy(part_ref.at[block(line.chips[order[k]]), :], mine.at[k], m_sem.at[k])

    for k in range(4):
        mine_copy(k).start()

    barrier = greet([{"tp": lax.rem(plane + i, n_tp)} for i in range(1, n_tp)]
                    + [{"dp": lax.rem(me + i, n_dp)} for i in range(1, n_dp)])

    @pl.when(jnp.logical_not(own))
    def _():
        pl.semaphore_signal(barrier, inc=1, device_id={"dp": owner, "tp": 0}, device_id_type=MESH)

    @pl.when(gathers_hot)
    def _():
        @pl.loop(0, per * n_dp)
        def _(k):
            dp, tp = lax.rem(k, n_dp), lax.div(k, n_dp) + me * per

            @pl.when(jnp.logical_not(jnp.logical_and(tp == 0, dp == me)))
            def _():
                pl.semaphore_signal(barrier, inc=1, device_id={"dp": dp, "tp": tp}, device_id_type=MESH)

    extra = jnp.where(own, 0, 1) + jnp.where(gathers_hot, per * n_dp - jnp.where(own, 1, 0), 0)
    pl.semaphore_wait(barrier, n_dp + n_tp - 2 + extra)

    def peer(i):
        return lax.rem(me + i, n_dp), lax.rem(me + n_dp - i, n_dp)

    def to_partner(k):
        return tp_copy(part_ref.at[block(line.other(line.chips[order[k]])), :], chip_sum.at[k],
                       (d_send, d_recv), k, line.partner)

    for k in range(4):
        to_partner(k).start()

    def idx_copy(i, to, slot):
        return pltpu.make_async_remote_copy(
            src_ref=send_ref.at[to], dst_ref=idx_ref.at[slot], send_sem=i_send.at[i], recv_sem=i_recv.at[i],
            device_id={"dp": to}, device_id_type=MESH)

    for i in range(1, n_dp):
        idx_copy(i, peer(i)[0], me).start()

    def add_chip(k):
        mine_copy(k).wait()
        to_partner(k).wait_recv()
        chip_sum[k] += mine[k]

    def half_copy(side, q):
        rows = pl.ds(side * half + q * PIECE, PIECE)
        return tp_copy(chip_sum.at[0, rows, :], half_in.at[side, pl.ds(q * PIECE, PIECE), :],
                       (h_send, h_recv), (side, q), (line.right, line.left)[side])

    def full_copy(side, q):
        rows = pl.ds(q * PIECE, PIECE)
        return tp_copy(chip_sum.at[1 + side, rows, :], full_in.at[side, rows, :],
                       (f_send, f_recv), (side, q), (line.right, line.left)[side])

    add_chip(0)
    for q in range(n_piece):
        for side in range(2):
            half_copy(side, q).start()
    add_chip(1)
    add_chip(2)
    for q in range(n_piece):
        full_copy(0, n_piece + q).start()
        full_copy(1, q).start()

    def n_rows(blk):
        return HOT_ROWS + cold_cap(plane, blk)

    for q in range(n_piece):
        for side in range(2):
            half_copy(side, q).wait_recv()
            rows = pl.ds(side * half + q * PIECE, PIECE)
            chip_sum[1 + side, rows, :] += half_in[side, pl.ds(q * PIECE, PIECE), :]
            full_copy(side, side * n_piece + q).start()
    add_chip(3)

    @pl.loop(0, n_slots // 128)
    def _(b):
        base = pl.multiple_of(b * 128, 128)
        rows = lax.broadcasted_iota(I32, (128, n_tok), 0) + base
        pick[pl.ds(base, 128), :] = (rows == slot_ref[...]).astype(BF16)

    @pl.loop(0, n_dp)
    def _(s):
        @pl.loop(lax.div(n_rows(me), 8), STRIDE // 8)
        def _(r):
            recv[s, pl.ds(pl.multiple_of(r * 8, 8), 8), :] = jnp.zeros((8, dim), F32)

    idx_ref[pl.ds(me, 1)] = send_ref[pl.ds(me, 1)]
    for i in range(1, n_dp):
        to, frm = peer(i)
        idx_copy(i, to, me).wait_send()
        idx_copy(i, frm, frm).wait_recv()

    @pl.loop(0, n_dp // 2)
    def _(p):
        lane = lax.broadcasted_iota(I32, (1, 128), 1)
        idx = jnp.where(lane < STRIDE, idx_ref[2 * p, 0:1, :], idx_ref[2 * p + 1, 0:1, :])
        rows = lax.broadcasted_iota(I32, (place.shape[0], 128), 0)
        place[:, pl.ds(pl.multiple_of(p * 128, 128), 128)] = (rows == idx).astype(BF16)

    gain = 1.0 + gain_ref[...]
    w_acc = jnp.zeros((8, dim), F32)
    for q in range(2 * n_piece):
        for side in range(2):
            full_copy(side, q).wait_recv()
        for r in range(q * PIECE, (q + 1) * PIECE, 8):
            rows = pl.ds(r, 8)
            total = (chip_sum[3, rows, :] + full_in[0, rows, :]) + full_in[1, rows, :]
            x_emb = total.astype(BF16)
            x_ref[rows, :] = x_emb
            x = x_emb.astype(F32)
            r_inv = lax.rsqrt(jnp.mean(x * x, axis=-1, keepdims=True) + NORM_EPS)
            x_hat = x * r_inv
            y_ref[rows, :] = (x_hat * gain).astype(BF16)
            dy = dyn_ref[rows, :].astype(F32)
            a = dy * gain
            g_ref[rows, :] = dyr_ref[rows, :].astype(F32) + r_inv * (a - x_hat * jnp.mean(a * x_hat, axis=-1, keepdims=True))
            w_acc = w_acc + dy * x_hat
    w_part[...] = jnp.sum(w_acc, axis=0, keepdims=True)

    def cols_of(c):
        return pl.ds(pl.multiple_of(c * wide, 128), wide)

    def ag_sent(kind, c):
        cols = cols_of(c)
        rows, to = (
            (block(plane), line.right), (block(plane), line.left),
            (block(line.left, 0, half), line.right), (block(line.right, half, half), line.left),
            (block(plane), line.partner), (block(line.left), line.partner),
            (block(line.right), line.partner), (block(line.opp), line.partner))[kind]
        src = g_ref.at[:, cols] if kind in (0, 1, 4) else g_all.at[rows, cols]
        return tp_copy(src, g_all.at[rows, cols], (ag_send, ag_recv), (kind, c), to)

    def ag_arrives(kind, c):
        cols = cols_of(c)
        rows = (block(line.left), block(line.right),
                block(line.opp, 0, half), block(line.opp, half, half),
                block(line.partner), block(line.other(line.left)),
                block(line.other(line.right)), block(line.other(line.opp)))[kind]
        return tp_copy(g_all.at[rows, cols], g_all.at[rows, cols], (ag_send, ag_recv), (kind, c), line.partner)

    def w_copy(i, slot):
        return pltpu.make_async_remote_copy(
            src_ref=w_part, dst_ref=w_dp.at[slot], send_sem=wd_send.at[i], recv_sem=wd_recv.at[i],
            device_id={"dp": peer(i)[0]}, device_id_type=MESH)

    def wt_copy(i, slot):
        return tp_copy(w_sum, w_tp.at[slot], (wt_send, wt_recv), i, lax.rem(plane + i, n_tp))

    def row_copy(c, i, size, to, slot):
        return pltpu.make_async_remote_copy(
            src_ref=send.at[pl.ds(pl.multiple_of(to * STRIDE, 8), size), cols_of(c)],
            dst_ref=recv.at[slot, pl.ds(0, size), cols_of(c)],
            send_sem=a_send.at[c, i], recv_sem=a_recv.at[c, i],
            device_id={"dp": to}, device_id_type=MESH)

    def by_size(want, fn):
        for size in sizes:
            @pl.when(want == size)
            def _():
                fn(size)

    at = pl.multiple_of(lax.rem(plane, per) * (n_dp * HOT_ROWS) + me * HOT_ROWS, 8)

    def hot_copy(c):
        return pltpu.make_async_remote_copy(
            src_ref=hot_send.at[:, cols_of(c)], dst_ref=hot_recv.at[pl.ds(at, HOT_ROWS), cols_of(c)],
            send_sem=hot_out.at[c], recv_sem=hot_in.at[0],
            device_id={"dp": owner, "tp": 0}, device_id_type=MESH)

    def send_own(c):
        for kind in (0, 1, 4):
            ag_sent(kind, c).start()

    send_own(0)
    send_own(1)
    for i in range(1, n_dp):
        w_copy(i, me).start()
    g_all[block(plane), :] = g_ref[...]

    @pl.loop(0, NCHUNK + 2 + LAG)
    def _(i):
        @pl.when(i + 2 < NCHUNK)
        def _():
            send_own(i + 2)

        @pl.when(i < NCHUNK)
        def _():
            ag_arrives(0, i).wait_recv()
            ag_sent(2, i).start()
            ag_sent(5, i).start()
            ag_arrives(1, i).wait_recv()
            ag_sent(3, i).start()
            ag_sent(6, i).start()

        @pl.when(jnp.logical_and(i >= 1, i < NCHUNK + 1))
        def _():
            ag_arrives(2, i - 1).wait_recv()
            ag_arrives(3, i - 1).wait_recv()
            ag_sent(7, i - 1).start()

        @pl.when(jnp.logical_and(i >= 2, i < NCHUNK + 2))
        def _():
            c = i - 2
            for kind in (4, 5, 6, 7):
                ag_arrives(kind, c).wait_recv()
            cols = cols_of(c)
            send[:, cols] = dot_exact(pick[...], g_all[:, cols])

            @pl.loop(1, n_dp)
            def _(k):
                to = peer(k)[0]
                by_size(n_rows(to), lambda size: row_copy(c, k, size, to, me).start())

            recv[pl.ds(me, 1), :, cols] = send[pl.ds(pl.multiple_of(me * STRIDE, 8), STRIDE), cols][None]

        @pl.when(i == 3)
        def _():
            w_dp[pl.ds(me, 1)] = w_part[...][None]
            for k in range(1, n_dp):
                w_copy(k, me).wait_send()
                w_copy(k, peer(k)[1]).wait_recv()
            w_sum[...] = jnp.sum(w_dp[...], axis=0)
            for k in range(1, n_tp):
                wt_copy(k, plane).start()
            w_tp[pl.ds(plane, 1)] = w_sum[...][None]

        @pl.when(i >= 2 + LAG)
        def _():
            c = i - 2 - LAG

            @pl.loop(1, n_dp)
            def _(k):
                to, frm = peer(k)
                by_size(n_rows(to), lambda size: row_copy(c, k, size, to, me).wait_send())
                by_size(n_rows(me), lambda size: row_copy(c, k, size, frm, frm).wait_recv())

            cols = cols_of(c)
            rows = recv[:, :, cols]
            hot_send[:, cols] = jnp.sum(rows[:, :HOT_ROWS, :], axis=0) * scale

            @pl.when(jnp.logical_not(own))
            def _():
                hot_copy(c).start()

            out_ref[:, cols] = dot_exact(place[...], rows.reshape(n_slots, wide)) * scale

    for i in range(1, n_tp):
        wt_copy(i, plane).wait_send()
        wt_copy(i, lax.rem(plane + n_tp - i, n_tp)).wait_recv()
    wout_ref[...] = jnp.sum(w_tp[...], axis=0)

    for k in range(4):
        to_partner(k).wait_send()
    for q in range(n_piece):
        for side in range(2):
            half_copy(side, q).wait_send()
    for q in range(2 * n_piece):
        for side in range(2):
            full_copy(side, q).wait_send()

    @pl.loop(0, NCHUNK)
    def _(c):
        for kind in range(8):
            ag_sent(kind, c).wait_send()

    @pl.when(jnp.logical_not(own))
    def _():
        @pl.loop(0, NCHUNK)
        def _(c):
            hot_copy(c).wait_send()

    def hot_wait(n):
        ref = hot_recv.at[pl.ds(0, n), :]
        pltpu.make_async_remote_copy(
            src_ref=ref, dst_ref=ref, send_sem=hot_out.at[0], recv_sem=hot_in.at[0],
            device_id={"dp": 1, "tp": 0}, device_id_type=MESH).wait_recv()

    total = hot_recv.shape[0]

    @pl.when(own)
    def _():
        hot_recv[0:HOT_ROWS, :] = hot_send[...]
        hot_wait(total - HOT_ROWS)

    @pl.when(jnp.logical_and(plane == 0, me == 1))
    def _():
        hot_wait(total)

    @pl.when(gathers_hot)
    def _():
        out_ref[...] += hot_recv[...]


def fused_step(n_dp, n_tp, out_rows, part, slot, send_idx, w_norm, dy_norm, dy_resid):
    n_pos, dim = dy_norm.shape
    n_tok = n_pos * n_tp
    half, pieces = n_pos // 2, n_pos // PIECE
    dma = pltpu.SemaphoreType.DMA
    vmem = pl.BlockSpec(memory_space=VMEM)
    shape = jax.ShapeDtypeStruct
    return pl.pallas_call(
        functools.partial(step_kernel, n_dp, n_tp),
        out_shape=(shape((n_pos, dim), BF16), shape((n_pos, dim), BF16), shape((n_pos, dim), F32),
                   shape((out_rows, dim), F32), shape((1, dim), F32), shape(send_idx.shape, I32)),
        in_specs=[pl.BlockSpec(memory_space=ANY)] + [vmem] * 5,
        out_specs=(vmem,) * 6,
        scratch_shapes=[
            VMEM((4, n_pos, dim), F32),
            VMEM((4, n_pos, dim), F32),
            VMEM((2, half, dim), F32),
            VMEM((2, n_pos, dim), F32),
            VMEM((n_tok, dim), F32),
            VMEM((n_dp * STRIDE, n_tok), BF16),
            VMEM((out_rows, n_dp * STRIDE), BF16),
            VMEM((n_dp * STRIDE, dim), F32),
            VMEM((n_dp, STRIDE, dim), F32),
            VMEM((HOT_ROWS, dim), F32),
            VMEM((HOT // 2, dim), F32),
            VMEM((1, dim), F32),
            VMEM((n_dp, 1, dim), F32),
            VMEM((1, dim), F32),
            VMEM((n_tp, 1, dim), F32),
            dma((4,)), dma((4,)), dma((4,)), dma((2, pieces // 2)), dma((2, pieces // 2)),
            dma((2, pieces)), dma((2, pieces)), dma((n_dp,)), dma((n_dp,)),
            dma((8, NCHUNK)), dma((8, NCHUNK)),
            dma((NCHUNK, n_dp)), dma((NCHUNK, n_dp)), dma((NCHUNK,)), dma((1,)),
            dma((n_dp,)), dma((n_dp,)), dma((n_tp,)), dma((n_tp,)),
        ],
        compiler_params=pltpu.CompilerParams(collective_id=1, has_side_effects=True, vmem_limit_bytes=67043328),
        name="fused_step",
    )(part, slot, send_idx, w_norm.reshape(1, dim), dy_norm, dy_resid)


def swap(x, axis):
    return lax.all_to_all(x, axis, split_axis=0, concat_axis=0)


def dense_grads(n_dp, n_tp, out_rows, tokens, g):
    g_all = swap(jnp.broadcast_to(g, (n_tp,) + g.shape), "tp").reshape(-1, g.shape[1])
    rows = n_dp * out_rows
    local = tokens - lax.axis_index("tp") * rows
    drop = jnp.where((local >= 0) & (local < rows), local, rows)
    shard = jax.ops.segment_sum(g_all, drop, num_segments=rows, mode="drop")
    return jnp.sum(swap(shard.reshape(n_dp, out_rows, -1), "dp"), axis=0) * math.sqrt(g.shape[1])


def route(n_dp, n_tp, out_rows, ids):
    plane = lax.axis_index("tp")
    n = ids.shape[0]
    cold = ids >= HOT
    bins = ids // out_rows
    hits = (bins[:, None] == jnp.arange(n_dp * n_tp)[None]) & cold[:, None]
    bin_no = jnp.arange(n_dp * n_tp)
    flag = jnp.any(jnp.sum(hits.astype(I32), axis=0) > cold_cap(bin_no // n_dp, bin_no % n_dp))
    blk = bins % n_dp
    mine = cold & (bins // n_dp == plane)
    block_hit = (blk[:, None] == jnp.arange(n_dp)[None]) & mine[:, None]
    before = (jnp.arange(n)[:, None] > jnp.arange(n)[None]).astype(BF16)
    rank = jnp.sum(jnp.where(block_hit, jnp.dot(before, block_hit.astype(BF16), preferred_element_type=F32), 0.0), axis=1).astype(I32)
    cold_slot = blk * STRIDE + HOT_ROWS + rank
    per_plane = HOT // n_tp
    in_plane = ids % per_plane
    hot_slot = (in_plane // HOT_ROWS) * STRIDE + in_plane % HOT_ROWS
    hot = jnp.logical_not(cold) & (ids // per_plane == plane)
    slot = jnp.where(mine, cold_slot, jnp.where(hot, hot_slot, -1))
    slots = jnp.arange(n_dp * STRIDE)
    row = jnp.max(jnp.where((slots[:, None] == slot[None]) & mine[None], (ids % out_rows)[None], -1), axis=1)
    row = row.reshape(n_dp, 1, STRIDE)
    row = jnp.concatenate([row, row], axis=2)
    send = jnp.where(jnp.arange(8)[None, :, None] == 1, flag.astype(I32), row)
    return slot.reshape(1, n), send


def solution(mesh):
    n_dp, n_tp = mesh.shape["dp"], mesh.shape["tp"]

    def local_step(tokens, emb_table, w_norm, dy_norm, dy_resid):
        shard_rows, dim = emb_table.shape
        out_rows = shard_rows // n_dp
        ids = tokens[0]
        slot, send_idx = route(n_dp, n_tp, out_rows, ids)
        local_ids = ids - lax.axis_index("tp") * shard_rows
        owned = (local_ids >= 0) & (local_ids < shard_rows)
        part = gather_rows(emb_table, local_ids, owned)
        x_emb, y_norm, g, emb_fast, w_sum, idx = fused_step(
            n_dp, n_tp, out_rows, part, slot, send_idx, w_norm, dy_norm[0], dy_resid[0])
        fits = jnp.max(idx[:, 1, :]) == 0
        emb_grad = lax.cond(fits, lambda: emb_fast, lambda: dense_grads(n_dp, n_tp, out_rows, ids, g))
        return x_emb[None], y_norm[None], emb_grad, w_sum[0]

    act_spec = P("dp", "tp", None)
    return jax.shard_map(local_step, mesh=mesh, in_specs=(P("dp", None), P("tp", None), P(None), act_spec, act_spec), out_specs=(act_spec, act_spec, P(("tp", "dp"), None), P(None)), check_vma=False)
```

```python
import functools
import math
import jax
import jax.numpy as jnp
from jax import lax
from jax.experimental import pallas as pl
from jax.experimental.pallas import tpu as pltpu
from jax.sharding import PartitionSpec as P

NORM_EPS = 1e-6
MESH = pl.DeviceIdType.MESH
HOT = 768
HOT_PLANE = 2
HOT_ROWS = 8
STRIDE = 64
SLOTS = 512
FRONT = 512
FAR = 320
NCHUNK = 9
LAG = 3
F32 = jnp.float32
BF16 = jnp.bfloat16
I32 = jnp.int32
VMEM = pltpu.VMEM
ANY = pl.ANY


def hot_rows(tp):
    return jnp.where(tp >= HOT_PLANE, HOT_ROWS, 0)


def cold_cap(tp, blk):
    first = jnp.where(blk == 0, 0, jnp.where(blk == 1, 40, jnp.where(blk < 4, 48, jnp.where(blk < 8, 32, 24))))
    return jnp.where(tp == 0, first, 16)


def slot_base(tp, blk):
    first = jnp.where(blk < 2, 0, jnp.where(blk < 4, 40 + 48 * (blk - 2), jnp.where(blk < 8, 136 + 32 * (blk - 4), 264 + 24 * (blk - 8))))
    return jnp.where(tp == 0, first, (16 + hot_rows(tp)) * blk)


def far_kernel(blk_ref, count_ref, table_ref, out_ref, sem):
    count = jnp.minimum(count_ref[0], FAR)
    out_ref[...] = jnp.zeros(out_ref.shape, BF16)

    def copy(i):
        return pltpu.make_async_copy(
            table_ref.at[pl.ds(pl.multiple_of(blk_ref[i] * 2, 2), 2), :],
            out_ref.at[pl.ds(pl.multiple_of(i * 2, 2), 2), :], sem)

    @pl.loop(0, count)
    def _(i):
        copy(i).start()

    @pl.loop(0, count)
    def _(i):
        copy(0).wait()


def far_rows(table, blk, count):
    return pl.pallas_call(
        far_kernel,
        out_shape=jax.ShapeDtypeStruct((2 * FAR, table.shape[1]), BF16),
        in_specs=[pl.BlockSpec(memory_space=pltpu.SMEM), pl.BlockSpec(memory_space=pltpu.SMEM),
                  pl.BlockSpec(memory_space=ANY)],
        out_specs=pl.BlockSpec(memory_space=VMEM),
        scratch_shapes=[pltpu.SemaphoreType.DMA],
        compiler_params=pltpu.CompilerParams(vmem_limit_bytes=16 * 2**20),
        name="far_rows",
    )(blk, count, table)


class Line:
    def __init__(self, n_tp):
        self.me = lax.axis_index("tp")
        n_chip = n_tp // 2
        chip, core = lax.div(self.me, 2), lax.rem(self.me, 2)
        self.core = core
        self.partner = chip * 2 + 1 - core
        self.left, self.right, self.opp = (
            lax.rem(chip + k, n_chip) * 2 + core for k in (n_chip - 1, 1, n_chip // 2))
        self.chips = {"opp": self.opp, "right": self.right, "left": self.left, "own": self.me}

    def other(self, tp):
        return tp + 1 - 2 * self.core


def tp_copy(src, dst, sems, at, tp):
    send, recv = sems
    return pltpu.make_async_remote_copy(
        src_ref=src, dst_ref=dst, send_sem=send.at[at], recv_sem=recv.at[at],
        device_id={"tp": tp}, device_id_type=MESH)


def greet(devices):
    barrier = pltpu.get_barrier_semaphore()
    for device in devices:
        pl.semaphore_signal(barrier, inc=1, device_id=device, device_id_type=MESH)
    return barrier


def split3(x):
    hi = x.astype(BF16)
    rest = x - hi.astype(F32)
    mid = rest.astype(BF16)
    return hi, mid, (rest - mid.astype(F32)).astype(BF16)


def dot_exact(one_hot, x):
    parts = [jnp.dot(one_hot, p, preferred_element_type=F32) for p in split3(x)]
    return (parts[2] + parts[1]) + parts[0]


def step_kernel(n_dp, n_tp, comb_ref, far_ref, front_ref, slot_ref, send_ref, gain_ref, dyn_ref, dyr_ref,
                x_ref, y_ref, out_ref, wout_ref, idx_ref,
                sel, mine, chip_sum, half_in, full_in, g_ref, g_all, pick, place, send, recv, hot_send, hot_recv,
                w_acc, w_part, w_dp, w_sum, w_tp,
                d_send, d_recv, h_send, h_recv, f_send, f_recv, i_send, i_recv,
                ag_send, ag_recv, a_send, a_recv, hot_out, hot_in, wd_send, wd_recv, wt_send, wt_recv):
    me, plane = lax.axis_index("dp"), lax.axis_index("tp")
    line = Line(n_tp)
    n_pos, dim = x_ref.shape
    half = n_pos // 2
    n_tok = n_pos * n_tp
    wide = dim // NCHUNK
    n_slots = n_dp * STRIDE
    scale = math.sqrt(dim)
    sizes = (16, 24, 32, 40, 48)
    order = ("opp", "right", "left", "own")
    per = out_ref.shape[0] // (n_dp * HOT_ROWS)
    is_hot = plane >= HOT_PLANE
    owner = lax.div(jnp.maximum(plane - HOT_PLANE, 0), per)
    gathers_hot = jnp.logical_and(plane == 0, me < 2)
    n_sources = jnp.where(me == 0, n_dp * per, n_dp * (n_tp - HOT_PLANE - per))

    def block(tp, start=0, size=n_pos):
        return pl.ds(pl.multiple_of(tp * n_pos + start, 8), size)

    barrier = greet([{"tp": lax.rem(plane + i, n_tp)} for i in range(1, n_tp)]
                    + [{"dp": lax.rem(me + i, n_dp)} for i in range(1, n_dp)])

    @pl.when(is_hot)
    def _():
        pl.semaphore_signal(barrier, inc=1, device_id={"dp": owner, "tp": 0}, device_id_type=MESH)

    @pl.when(gathers_hot)
    def _():
        @pl.loop(0, n_sources)
        def _(k):
            tp = HOT_PLANE + per * me + lax.div(k, n_dp)
            pl.semaphore_signal(barrier, inc=1, device_id={"dp": lax.rem(k, n_dp), "tp": tp}, device_id_type=MESH)

    extra = jnp.where(is_hot, 1, 0) + jnp.where(gathers_hot, n_sources, 0)
    pl.semaphore_wait(barrier, n_dp + n_tp - 2 + extra)

    def peer(i):
        return lax.rem(me + i, n_dp), lax.rem(me + n_dp - i, n_dp)

    def cols_of(c):
        return pl.ds(pl.multiple_of(c * wide, 128), wide)

    def idx_copy(i, to, slot):
        return pltpu.make_async_remote_copy(
            src_ref=send_ref.at[to], dst_ref=idx_ref.at[slot], send_sem=i_send.at[i], recv_sem=i_recv.at[i],
            device_id={"dp": to}, device_id_type=MESH)

    for i in range(1, n_dp):
        idx_copy(i, peer(i)[0], me).start()

    def to_partner(k, c):
        return tp_copy(send.at[pl.ds(k * n_pos, n_pos), cols_of(c)], chip_sum.at[k, :, cols_of(c)],
                       (d_send, d_recv), (k, c), line.partner)

    def look_up(k):
        mine_tp = line.chips[order[k]]
        for part, tp in enumerate((line.other(mine_tp), mine_tp)):
            lanes = lax.broadcasted_iota(I32, (n_pos, sel.shape[1]), 1)
            sel[pl.ds(part * n_pos, n_pos), :] = (lanes == comb_ref[block(tp), :]).astype(BF16)

        @pl.loop(0, NCHUNK)
        def _(c):
            cols = cols_of(c)
            rows = jnp.dot(sel[:, :FRONT], front_ref[:, cols], preferred_element_type=F32)
            rows = (rows + jnp.dot(sel[:, FRONT:], far_ref[:, cols], preferred_element_type=F32)) * scale
            send[pl.ds(k * n_pos, n_pos), cols] = rows[:n_pos]
            mine[k, :, cols] = rows[n_pos:]
            to_partner(k, c).start()

    def add_chip(k, c):
        to_partner(k, c).wait_recv()
        chip_sum[k, :, cols_of(c)] += mine[k, :, cols_of(c)]

    def half_copy(side, c):
        return tp_copy(chip_sum.at[0, pl.ds(side * half, half), cols_of(c)], half_in.at[side, :, cols_of(c)],
                       (h_send, h_recv), (side, c), (line.right, line.left)[side])

    def full_copy(side, part, c):
        rows = pl.ds(part * half, half)
        return tp_copy(chip_sum.at[1 + side, rows, cols_of(c)], full_in.at[side, rows, cols_of(c)],
                       (f_send, f_recv), (2 * side + part, c), (line.right, line.left)[side])

    look_up(0)

    @pl.loop(0, NCHUNK)
    def _(c):
        add_chip(0, c)
        for side in range(2):
            half_copy(side, c).start()

    look_up(1)
    look_up(2)

    @pl.loop(0, NCHUNK)
    def _(c):
        add_chip(1, c)
        full_copy(0, 1, c).start()
        add_chip(2, c)
        full_copy(1, 0, c).start()

    @pl.loop(0, NCHUNK)
    def _(c):
        for side in range(2):
            half_copy(side, c).wait_recv()
            chip_sum[1 + side, pl.ds(side * half, half), cols_of(c)] += half_in[side, :, cols_of(c)]
            full_copy(side, side, c).start()

    look_up(3)

    def n_rows(blk):
        return hot_rows(plane) + cold_cap(plane, blk)

    @pl.loop(0, SLOTS // 128)
    def _(b):
        base = pl.multiple_of(b * 128, 128)
        rows = lax.broadcasted_iota(I32, (128, n_tok), 0) + base
        pick[pl.ds(base, 128), :] = (rows == slot_ref[...]).astype(BF16)

    @pl.loop(0, n_dp)
    def _(s):
        @pl.loop(lax.div(n_rows(me), 8), STRIDE // 8)
        def _(r):
            recv[s, pl.ds(pl.multiple_of(r * 8, 8), 8), :] = jnp.zeros((8, dim), F32)

    idx_ref[pl.ds(me, 1)] = send_ref[pl.ds(me, 1)]
    for i in range(1, n_dp):
        to, frm = peer(i)
        idx_copy(i, to, me).wait_send()
        idx_copy(i, frm, frm).wait_recv()

    @pl.loop(0, n_dp // 2)
    def _(p):
        lane = lax.broadcasted_iota(I32, (1, 128), 1)
        idx = jnp.where(lane < STRIDE, idx_ref[2 * p, 0:1, :], idx_ref[2 * p + 1, 0:1, :])
        rows = lax.broadcasted_iota(I32, (place.shape[0], 128), 0)
        place[:, pl.ds(pl.multiple_of(p * 128, 128), 128)] = (rows == idx).astype(BF16)

    gain = 1.0 + gain_ref[...]
    w_acc[...] = jnp.zeros(w_acc.shape, F32)

    @pl.loop(0, NCHUNK)
    def _(c):
        add_chip(3, c)
        for side in range(2):
            for part in range(2):
                full_copy(side, part, c).wait_recv()

        for k in range(4):
            to_partner(k, c).wait_send()

    @pl.loop(0, n_pos // 16)
    def _(q):
        for r in range(2):
            rows = pl.ds(pl.multiple_of(q * 16 + r * 8, 8), 8)
            total = (chip_sum[3, rows, :] + full_in[0, rows, :]) + full_in[1, rows, :]
            x_emb = total.astype(BF16)
            x_ref[rows, :] = x_emb
            x = x_emb.astype(F32)
            r_inv = lax.rsqrt(jnp.mean(x * x, axis=-1, keepdims=True) + NORM_EPS)
            x_hat = x * r_inv
            y_ref[rows, :] = (x_hat * gain).astype(BF16)
            dy = dyn_ref[rows, :].astype(F32)
            a = dy * gain
            g_ref[rows, :] = dyr_ref[rows, :].astype(F32) + r_inv * (a - x_hat * jnp.mean(a * x_hat, axis=-1, keepdims=True))
            w_acc[...] += dy * x_hat

    w_part[...] = jnp.sum(w_acc[...], axis=0, keepdims=True)

    def ag_sent(kind, c):
        cols = cols_of(c)
        rows, to = (
            (block(plane), line.right), (block(plane), line.left),
            (block(line.left, 0, half), line.right), (block(line.right, half, half), line.left),
            (block(plane), line.partner), (block(line.left), line.partner),
            (block(line.right), line.partner), (block(line.opp), line.partner))[kind]
        src = g_ref.at[:, cols] if kind in (0, 1, 4) else g_all.at[rows, cols]
        return tp_copy(src, g_all.at[rows, cols], (ag_send, ag_recv), (kind, c), to)

    def ag_arrives(kind, c):
        cols = cols_of(c)
        rows = (block(line.left), block(line.right),
                block(line.opp, 0, half), block(line.opp, half, half),
                block(line.partner), block(line.other(line.left)),
                block(line.other(line.right)), block(line.other(line.opp)))[kind]
        return tp_copy(g_all.at[rows, cols], g_all.at[rows, cols], (ag_send, ag_recv), (kind, c), line.partner)

    def w_copy(i, slot):
        return pltpu.make_async_remote_copy(
            src_ref=w_part, dst_ref=w_dp.at[slot], send_sem=wd_send.at[i], recv_sem=wd_recv.at[i],
            device_id={"dp": peer(i)[0]}, device_id_type=MESH)

    def wt_copy(i, slot):
        return tp_copy(w_sum, w_tp.at[slot], (wt_send, wt_recv), i, lax.rem(plane + i, n_tp))

    def row_copy(c, i, size, to, slot):
        return pltpu.make_async_remote_copy(
            src_ref=send.at[pl.ds(pl.multiple_of(slot_base(plane, to), 8), size), cols_of(c)],
            dst_ref=recv.at[slot, pl.ds(0, size), cols_of(c)],
            send_sem=a_send.at[c, i], recv_sem=a_recv.at[c, i],
            device_id={"dp": to}, device_id_type=MESH)

    def by_size(want, fn):
        for size in sizes:
            @pl.when(want == size)
            def _():
                fn(size)

    at = pl.multiple_of(lax.rem(jnp.maximum(plane - HOT_PLANE, 0), per) * (n_dp * HOT_ROWS) + me * HOT_ROWS, 8)

    def hot_copy(c):
        return pltpu.make_async_remote_copy(
            src_ref=hot_send.at[:, cols_of(c)], dst_ref=hot_recv.at[pl.ds(at, HOT_ROWS), cols_of(c)],
            send_sem=hot_out.at[c], recv_sem=hot_in.at[0],
            device_id={"dp": owner, "tp": 0}, device_id_type=MESH)

    def send_own(c):
        for kind in (0, 1, 4):
            ag_sent(kind, c).start()

    send_own(0)
    send_own(1)
    for i in range(1, n_dp):
        w_copy(i, me).start()
    g_all[block(plane), :] = g_ref[...]

    @pl.loop(0, NCHUNK + 2 + LAG)
    def _(i):
        @pl.when(i + 2 < NCHUNK)
        def _():
            send_own(i + 2)

        @pl.when(i < NCHUNK)
        def _():
            ag_arrives(0, i).wait_recv()
            ag_sent(2, i).start()
            ag_sent(5, i).start()
            ag_arrives(1, i).wait_recv()
            ag_sent(3, i).start()
            ag_sent(6, i).start()

        @pl.when(jnp.logical_and(i >= 1, i < NCHUNK + 1))
        def _():
            ag_arrives(2, i - 1).wait_recv()
            ag_arrives(3, i - 1).wait_recv()
            ag_sent(7, i - 1).start()

        @pl.when(jnp.logical_and(i >= 2, i < NCHUNK + 2))
        def _():
            c = i - 2
            for kind in (4, 5, 6, 7):
                ag_arrives(kind, c).wait_recv()
            cols = cols_of(c)
            send[:, cols] = dot_exact(pick[...], g_all[:, cols])

            @pl.loop(1, n_dp)
            def _(k):
                to = peer(k)[0]
                by_size(n_rows(to), lambda size: row_copy(c, k, size, to, me).start())

            def keep(size):
                recv[pl.ds(me, 1), :size, cols] = send[pl.ds(pl.multiple_of(slot_base(plane, me), 8), size), cols][None]

            by_size(n_rows(me), keep)

        @pl.when(i == 3)
        def _():
            w_dp[pl.ds(me, 1)] = w_part[...][None]
            for k in range(1, n_dp):
                w_copy(k, me).wait_send()
                w_copy(k, peer(k)[1]).wait_recv()
            w_sum[...] = jnp.sum(w_dp[...], axis=0)
            for k in range(1, n_tp):
                wt_copy(k, plane).start()
            w_tp[pl.ds(plane, 1)] = w_sum[...][None]

        @pl.when(i >= 2 + LAG)
        def _():
            c = i - 2 - LAG

            @pl.loop(1, n_dp)
            def _(k):
                to, frm = peer(k)
                by_size(n_rows(to), lambda size: row_copy(c, k, size, to, me).wait_send())
                by_size(n_rows(me), lambda size: row_copy(c, k, size, frm, frm).wait_recv())

            cols = cols_of(c)
            rows = recv[:, :, cols]

            @pl.when(is_hot)
            def _():
                hot_send[:, cols] = jnp.sum(rows[:, :HOT_ROWS, :], axis=0) * scale
                hot_copy(c).start()

            out_ref[:, cols] = dot_exact(place[...], rows.reshape(n_slots, wide)) * scale

    for i in range(1, n_tp):
        wt_copy(i, plane).wait_send()
        wt_copy(i, lax.rem(plane + n_tp - i, n_tp)).wait_recv()
    wout_ref[...] = jnp.sum(w_tp[...], axis=0)

    @pl.loop(0, NCHUNK)
    def _(c):
        for side in range(2):
            half_copy(side, c).wait_send()
            for part in range(2):
                full_copy(side, part, c).wait_send()

    @pl.loop(0, NCHUNK)
    def _(c):
        for kind in range(8):
            ag_sent(kind, c).wait_send()

    @pl.when(is_hot)
    def _():
        @pl.loop(0, NCHUNK)
        def _(c):
            hot_copy(c).wait_send()

    def take_hot(n):
        ref = hot_recv.at[pl.ds(0, n), :]
        pltpu.make_async_remote_copy(
            src_ref=ref, dst_ref=ref, send_sem=hot_out.at[0], recv_sem=hot_in.at[0],
            device_id={"dp": 2, "tp": 0}, device_id_type=MESH).wait_recv()
        out_ref[pl.ds(0, n), :] += hot_recv[pl.ds(0, n), :]

    total = hot_recv.shape[0]

    @pl.when(jnp.logical_and(plane == 0, me == 0))
    def _():
        take_hot(total)

    @pl.when(jnp.logical_and(plane == 0, me == 1))
    def _():
        take_hot(HOT - total)


def fused_step(n_dp, n_tp, out_rows, comb, far, table, slot, send_idx, w_norm, dy_norm, dy_resid):
    n_pos, dim = dy_norm.shape
    n_tok = n_pos * n_tp
    half = n_pos // 2
    dma = pltpu.SemaphoreType.DMA
    vmem = pl.BlockSpec(memory_space=VMEM)
    shape = jax.ShapeDtypeStruct
    return pl.pallas_call(
        functools.partial(step_kernel, n_dp, n_tp),
        grid=(1,),
        out_shape=(shape((n_pos, dim), BF16), shape((n_pos, dim), BF16),
                   shape((out_rows, dim), F32), shape((1, dim), F32), shape(send_idx.shape, I32)),
        in_specs=[vmem, vmem, pl.BlockSpec((FRONT, dim), lambda i: (0, 0), pipeline_mode=pl.Buffered(1))] + [vmem] * 5,
        out_specs=(vmem,) * 5,
        scratch_shapes=[
            VMEM((2 * n_pos, FRONT + 2 * FAR), BF16),
            VMEM((4, n_pos, dim), F32),
            VMEM((4, n_pos, dim), F32),
            VMEM((2, half, dim), F32),
            VMEM((2, n_pos, dim), F32),
            VMEM((n_pos, dim), F32),
            VMEM((n_tok, dim), F32),
            VMEM((SLOTS, n_tok), BF16),
            VMEM((out_rows, n_dp * STRIDE), BF16),
            VMEM((SLOTS, dim), F32),
            VMEM((n_dp, STRIDE, dim), F32),
            VMEM((HOT_ROWS, dim), F32),
            VMEM((out_rows, dim), F32),
            VMEM((8, dim), F32),
            VMEM((1, dim), F32),
            VMEM((n_dp, 1, dim), F32),
            VMEM((1, dim), F32),
            VMEM((n_tp, 1, dim), F32),
            dma((4, NCHUNK)), dma((4, NCHUNK)), dma((2, NCHUNK)), dma((2, NCHUNK)),
            dma((4, NCHUNK)), dma((4, NCHUNK)), dma((n_dp,)), dma((n_dp,)),
            dma((8, NCHUNK)), dma((8, NCHUNK)),
            dma((NCHUNK, n_dp)), dma((NCHUNK, n_dp)), dma((NCHUNK,)), dma((1,)),
            dma((n_dp,)), dma((n_dp,)), dma((n_tp,)), dma((n_tp,)),
        ],
        compiler_params=pltpu.CompilerParams(collective_id=1, has_side_effects=True, vmem_limit_bytes=67043328),
        name="fused_step",
    )(comb, far, table, slot, send_idx, w_norm.reshape(1, dim), dy_norm, dy_resid)


def swap(x, axis):
    return lax.all_to_all(x, axis, split_axis=0, concat_axis=0)


def dense_step(n_dp, n_tp, out_rows, ids, table, w_norm, dy_norm, dy_resid):
    dim = table.shape[1]
    rows = table.shape[0]
    scale = math.sqrt(dim)
    local = ids - lax.axis_index("tp") * rows
    owned = (local >= 0) & (local < rows)
    looked = jnp.take(table, jnp.where(owned, local, 0), axis=0).astype(F32) * scale
    part = jnp.where(owned[:, None], looked, 0.0).reshape((n_tp,) + dy_norm.shape)
    x_emb = jnp.sum(swap(part, "tp"), axis=0).astype(BF16)
    x = x_emb.astype(F32)
    r_inv = lax.rsqrt(jnp.mean(x * x, axis=-1, keepdims=True) + NORM_EPS)
    x_hat = x * r_inv
    gain = 1.0 + w_norm
    y_norm = (x_hat * gain).astype(BF16)
    dy = dy_norm.astype(F32)
    a = dy * gain
    g = dy_resid.astype(F32) + r_inv * (a - x_hat * jnp.mean(a * x_hat, axis=-1, keepdims=True))
    w = jnp.sum(dy * x_hat, axis=0)[None]
    w = jnp.sum(swap(jnp.broadcast_to(w, (n_dp,) + w.shape), "dp"), axis=0)
    w = jnp.sum(swap(jnp.broadcast_to(w, (n_tp,) + w.shape), "tp"), axis=0)
    g_all = swap(jnp.broadcast_to(g, (n_tp,) + g.shape), "tp").reshape(-1, dim)
    shard = jax.ops.segment_sum(g_all, jnp.where(owned, local, rows), num_segments=rows, mode="drop")
    emb = jnp.sum(swap(shard.reshape(n_dp, out_rows, -1), "dp"), axis=0) * scale
    return x_emb, y_norm, emb, w


def route(n_dp, n_tp, out_rows, ids):
    plane = lax.axis_index("tp")
    n = ids.shape[0]
    shard_rows = n_dp * out_rows
    local = ids - plane * shard_rows
    owned = (local >= 0) & (local < shard_rows)
    far = owned & (local >= FRONT)
    cold = ids >= HOT
    mine = cold & owned
    blk = (ids // out_rows) % n_dp
    marks = jnp.concatenate([(blk[:, None] == jnp.arange(n_dp)[None]) & mine[:, None], far[:, None]], axis=1)
    before = (jnp.arange(n)[:, None] > jnp.arange(n)[None]).astype(BF16)
    ranks = jnp.dot(before, marks.astype(BF16), preferred_element_type=F32)
    rank = jnp.sum(jnp.where(marks, ranks, 0.0)[:, :n_dp], axis=1).astype(I32)
    far_rank = ranks[:, n_dp].astype(I32)
    comb = jnp.where(far, FRONT + far_rank * 2 + (local & 1), jnp.where(owned, local, -1))
    hit = (jnp.arange(FAR)[:, None] == far_rank[None]) & far[None]
    pair = jnp.max(jnp.where(hit, (local >> 1)[None], 0), axis=1)
    count = jnp.sum(far.astype(I32)).reshape(1)
    cold_slot = slot_base(plane, blk) + hot_rows(plane) + rank
    per_plane = n_dp * HOT_ROWS
    in_plane = ids % per_plane
    hot_slot = slot_base(plane, in_plane // HOT_ROWS) + in_plane % HOT_ROWS
    hot = jnp.logical_not(cold) & (ids // per_plane == plane - HOT_PLANE)
    slot = jnp.where(mine, cold_slot, jnp.where(hot, hot_slot, -1))
    d, c = jnp.arange(n_dp)[:, None], jnp.arange(STRIDE)[None]
    size = hot_rows(plane) + cold_cap(plane, d)
    at = jnp.where(c < size, slot_base(plane, d) + c, -2).reshape(-1)
    row = jnp.max(jnp.where((at[:, None] == slot[None]) & mine[None], (ids % out_rows)[None], -1), axis=1)
    row = row.reshape(n_dp, 1, STRIDE)
    row = jnp.concatenate([row, row], axis=2)
    bin_no = jnp.arange(n_dp * n_tp)
    hits = ((ids // out_rows)[:, None] == bin_no[None]) & cold[:, None]
    flag = jnp.any(jnp.sum(hits.astype(I32), axis=0) > cold_cap(bin_no // n_dp, bin_no % n_dp))
    all_far = ((ids // shard_rows)[:, None] == jnp.arange(n_tp)[None]) & (ids % shard_rows >= FRONT)[:, None]
    flag = flag | jnp.any(jnp.sum(all_far.astype(I32), axis=0) > FAR)
    send = jnp.where(jnp.arange(8)[None, :, None] == 1, flag.astype(I32), row)
    return comb.reshape(n, 1), pair, count, slot.reshape(1, n), send


def solution(mesh):
    n_dp, n_tp = mesh.shape["dp"], mesh.shape["tp"]

    def local_step(tokens, emb_table, w_norm, dy_norm, dy_resid):
        out_rows = emb_table.shape[0] // n_dp
        ids = tokens[0]
        comb, pair, count, slot, send_idx = route(n_dp, n_tp, out_rows, ids)
        far = far_rows(emb_table, pair, count)
        *fast, idx = fused_step(n_dp, n_tp, out_rows, comb, far, emb_table, slot, send_idx, w_norm, dy_norm[0], dy_resid[0])
        fits = jnp.max(idx[:, 1, :]) == 0
        x_emb, y_norm, emb_grad, w_sum = lax.cond(
            fits,
            lambda: tuple(fast),
            lambda: dense_step(n_dp, n_tp, out_rows, ids, emb_table, w_norm, dy_norm[0], dy_resid[0]),
        )
        return x_emb[None], y_norm[None], emb_grad, w_sum[0]

    act_spec = P("dp", "tp", None)
    return jax.shard_map(local_step, mesh=mesh, in_specs=(P("dp", None), P("tp", None), P(None), act_spec, act_spec), out_specs=(act_spec, act_spec, P(("tp", "dp"), None), P(None)), check_vma=False)
```

```python
import functools
import math
import jax
import jax.numpy as jnp
from jax import lax
from jax.experimental import pallas as pl
from jax.experimental.pallas import tpu as pltpu
from jax.sharding import PartitionSpec as P

NORM_EPS = 1e-6
MESH = pl.DeviceIdType.MESH
HOT = 768
HOT_PLANE = 2
HOT_ROWS = 8
STRIDE = 64
SLOTS = 512
FRONT = 512
FAR = 320
NCHUNK = 9
LAG = 3
F32 = jnp.float32
BF16 = jnp.bfloat16
I32 = jnp.int32
VMEM = pltpu.VMEM
ANY = pl.ANY


def hot_rows(tp):
    return jnp.where(tp >= HOT_PLANE, HOT_ROWS, 0)


def cold_cap(tp, blk):
    first = jnp.where(blk == 0, 0, jnp.where(blk == 1, 40, jnp.where(blk < 4, 48, jnp.where(blk < 8, 32, 24))))
    return jnp.where(tp == 0, first, 16)


def slot_base(tp, blk):
    first = jnp.where(blk < 2, 0, jnp.where(blk < 4, 40 + 48 * (blk - 2), jnp.where(blk < 8, 136 + 32 * (blk - 4), 264 + 24 * (blk - 8))))
    return jnp.where(tp == 0, first, (16 + hot_rows(tp)) * blk)


def plan_kernel(n_dp, n_tp, ids_ref, table_ref, comb_ref, far_ref, slot_ref, send_ref,
                before, hits, pairs, pairs_smem, sem, far_sem):
    plane = lax.axis_index("tp")
    n = ids_ref.shape[1]
    shard_rows = table_ref.shape[0]
    out_rows = shard_rows // n_dp
    ids = ids_ref[...]
    local = ids - plane * shard_rows
    owned = jnp.logical_and(local >= 0, local < shard_rows)
    far = jnp.logical_and(owned, local >= FRONT)
    cold = ids >= HOT
    mine = jnp.logical_and(cold, owned)
    bins = lax.div(ids, out_rows)
    blk = lax.rem(bins, n_dp)
    far_ref[...] = jnp.zeros(far_ref.shape, BF16)

    @pl.loop(0, n // 128)
    def _(b):
        base = pl.multiple_of(b * 128, 128)
        row = lax.broadcasted_iota(I32, (128, n), 0) + base
        before[pl.ds(base, 128), :] = (row < lax.broadcasted_iota(I32, (128, n), 1)).astype(BF16)

    kind = lax.broadcasted_iota(I32, (2 * n_dp, n), 0)
    mark = jnp.logical_or(jnp.logical_and(kind == blk, mine), jnp.logical_and(kind == n_dp, far))
    ranks = jnp.dot(mark.astype(BF16), before[...], preferred_element_type=F32)
    rank = jnp.sum(jnp.where(jnp.logical_and(mark, kind < n_dp), ranks, 0.0), axis=0, keepdims=True).astype(I32)
    far_rank = jnp.sum(jnp.where(jnp.logical_and(mark, kind == n_dp), ranks, 0.0), axis=0, keepdims=True).astype(I32)
    count = jnp.sum(far.astype(F32))

    comb = jnp.where(far, FRONT + far_rank * 2 + lax.rem(local, 2), jnp.where(owned, local, -1))
    place = hot_rows(plane) + rank
    per_plane = n_dp * HOT_ROWS
    in_plane = lax.rem(ids, per_plane)
    hot_slot = slot_base(plane, lax.div(in_plane, HOT_ROWS)) + lax.rem(in_plane, HOT_ROWS)
    hot = jnp.logical_and(jnp.logical_not(cold), lax.div(ids, per_plane) == plane - HOT_PLANE)
    slot_ref[...] = jnp.where(mine, slot_base(plane, blk) + place, jnp.where(hot, hot_slot, -1))

    wide_slot = jnp.where(jnp.logical_and(mine, place < STRIDE), blk * STRIDE + place, -1)
    far_slot = jnp.where(far, far_rank, -1)
    sub = lax.broadcasted_iota(I32, (8, n), 0)
    stack = jnp.where(sub == 0, comb, jnp.where(sub == 1, wide_slot, jnp.where(sub == 2, far_slot, bins)))
    stack = jnp.where(jnp.logical_and(sub == 4, jnp.logical_not(cold)), -1, stack)
    in_front = lax.rem(ids, shard_rows) < FRONT
    stack = jnp.where(sub == 5, jnp.where(in_front, -1, lax.div(ids, shard_rows)), stack)
    cols = jnp.transpose(stack.astype(F32)).astype(I32)
    comb_ref[...] = cols

    half = lax.div(local, 2)
    row = lax.rem(ids, out_rows)
    vals = jnp.where(sub == 0, lax.rem(half, 64), jnp.where(sub == 1, lax.div(half, 64), jnp.where(
        sub == 2, lax.rem(row, 16), jnp.where(sub == 3, lax.div(row, 16), 1))))
    vals = vals.astype(F32).astype(BF16)

    def pull(at, width):
        @pl.loop(0, n // 128)
        def _(b):
            rows = pl.ds(pl.multiple_of(b * 128, 128), 128)
            lane = lax.broadcasted_iota(I32, (128, width), 1)
            hits[rows, :width] = (lane == comb_ref[rows, at:at + 1]).astype(BF16)
        return jnp.dot(vals, hits[:, :width], preferred_element_type=F32)

    found = pull(2, pairs.shape[1])
    pick = found[1:2, :] * 64.0 + found[0:1, :]
    which = lax.broadcasted_iota(I32, pairs.shape, 0)
    pairs[...] = jnp.where(which == 0, pick, jnp.minimum(count, 1.0 * FAR)).astype(I32)
    move = pltpu.make_async_copy(pairs, pairs_smem, sem)
    move.start()
    move.wait()
    n_far = pairs_smem[1, 0]

    def far_copy(src, i):
        return pltpu.make_async_copy(
            table_ref.at[pl.ds(pl.multiple_of(src * 2, 2), 2), :],
            far_ref.at[pl.ds(pl.multiple_of(i * 2, 2), 2), :], far_sem)

    @pl.loop(0, n_far)
    def _(i):
        far_copy(pairs_smem[0, i], i).start()

    found = pull(1, n_dp * STRIDE)
    taken = found[4:5, :] > 0.5
    idx = jnp.where(taken, (found[3:4, :] * 16.0 + found[2:3, :]).astype(I32), -1)

    lane = lax.broadcasted_iota(I32, (n, 128), 1)
    in_bin = jnp.sum(jnp.where(lane == cols[:, 4:5], 1.0, 0.0), axis=0, keepdims=True)
    in_far = jnp.sum(jnp.where(lane == cols[:, 5:6], 1.0, 0.0), axis=0, keepdims=True)
    bin_no = lax.broadcasted_iota(I32, (1, 128), 1)
    cap = cold_cap(lax.div(bin_no, n_dp), lax.rem(bin_no, n_dp)).astype(F32)
    over = jnp.logical_or(in_bin > cap, in_far > 1.0 * FAR)
    flag = jnp.broadcast_to(jnp.max(jnp.where(over, 1.0, 0.0), axis=1, keepdims=True), (1, 128)).astype(I32)
    which = lax.broadcasted_iota(I32, (8, 128), 0)
    for p in range(n_dp // 2):
        send_ref[p] = jnp.where(which == 1, flag, idx[:, p * 128:(p + 1) * 128])

    @pl.loop(0, n_far)
    def _(i):
        far_copy(0, i).wait()


def make_plan(n_dp, n_tp, ids, table):
    n = ids.shape[1]
    vmem = pl.BlockSpec(memory_space=VMEM)
    shape = jax.ShapeDtypeStruct
    dma = pltpu.SemaphoreType.DMA
    n_pairs = FAR + -FAR % 128
    return pl.pallas_call(
        functools.partial(plan_kernel, n_dp, n_tp),
        out_shape=(shape((n, 8), I32), shape((2 * FAR, table.shape[1]), BF16),
                   shape((1, n), I32), shape((n_dp // 2, 8, 128), I32)),
        in_specs=[vmem, pl.BlockSpec(memory_space=ANY)],
        out_specs=(vmem,) * 4,
        scratch_shapes=[
            VMEM((n, n), BF16),
            VMEM((n, n_dp * STRIDE), BF16),
            VMEM((8, n_pairs), I32),
            pltpu.SMEM((8, n_pairs), I32),
            dma, dma,
        ],
        compiler_params=pltpu.CompilerParams(vmem_limit_bytes=24 * 2**20),
        name="make_plan",
    )(ids, table)


def copy_kernel(x_ref, y_ref, e_ref, xo_ref, yo_ref, eo_ref):
    xo_ref[...] = x_ref[...]
    yo_ref[...] = y_ref[...]
    eo_ref[...] = e_ref[...]


def hand_on(x, y, e):
    steps = 8
    specs = [pl.BlockSpec((a.shape[0] // steps, a.shape[1]), lambda i: (i, 0)) for a in (x, y, e)]
    return pl.pallas_call(
        copy_kernel,
        grid=(steps,),
        out_shape=tuple(jax.ShapeDtypeStruct(a.shape, a.dtype) for a in (x, y, e)),
        in_specs=specs,
        out_specs=tuple(specs),
        compiler_params=pltpu.CompilerParams(vmem_limit_bytes=8 * 2**20),
        name="hand_on",
    )(x, y, e)


class Line:
    def __init__(self, n_tp):
        self.me = lax.axis_index("tp")
        n_chip = n_tp // 2
        chip, core = lax.div(self.me, 2), lax.rem(self.me, 2)
        self.core = core
        self.partner = chip * 2 + 1 - core
        self.left, self.right, self.opp = (
            lax.rem(chip + k, n_chip) * 2 + core for k in (n_chip - 1, 1, n_chip // 2))
        self.chips = {"opp": self.opp, "right": self.right, "left": self.left, "own": self.me}

    def other(self, tp):
        return tp + 1 - 2 * self.core


def tp_copy(src, dst, sems, at, tp):
    send, recv = sems
    return pltpu.make_async_remote_copy(
        src_ref=src, dst_ref=dst, send_sem=send.at[at], recv_sem=recv.at[at],
        device_id={"tp": tp}, device_id_type=MESH)


def greet(devices):
    barrier = pltpu.get_barrier_semaphore()
    for device in devices:
        pl.semaphore_signal(barrier, inc=1, device_id=device, device_id_type=MESH)
    return barrier


def split3(x):
    hi = x.astype(BF16)
    rest = x - hi.astype(F32)
    mid = rest.astype(BF16)
    return hi, mid, (rest - mid.astype(F32)).astype(BF16)


def dot_exact(one_hot, x):
    parts = [jnp.dot(one_hot, p, preferred_element_type=F32) for p in split3(x)]
    return (parts[2] + parts[1]) + parts[0]


def step_kernel(n_dp, n_tp, comb_ref, far_ref, front_ref, slot_ref, send_ref, gain_ref, dyn_ref, dyr_ref,
                x_ref, y_ref, out_ref, wout_ref, flag_ref,
                idx_ref, sel, mine, chip_sum, half_in, full_in, g_ref, g_all, pick, place, send, recv, hot_send, hot_recv,
                w_acc, w_part, w_dp, w_sum, w_tp,
                d_send, d_recv, h_send, h_recv, f_send, f_recv, i_send, i_recv,
                ag_send, ag_recv, a_send, a_recv, hot_out, hot_in, wd_send, wd_recv, wt_send, wt_recv):
    me, plane = lax.axis_index("dp"), lax.axis_index("tp")
    line = Line(n_tp)
    n_pos, dim = x_ref.shape
    half = n_pos // 2
    n_tok = n_pos * n_tp
    wide = dim // NCHUNK
    n_slots = n_dp * STRIDE
    scale = math.sqrt(dim)
    sizes = (16, 24, 32, 40, 48)
    order = ("opp", "right", "left", "own")
    per = out_ref.shape[0] // (n_dp * HOT_ROWS)
    is_hot = plane >= HOT_PLANE
    owner = lax.div(jnp.maximum(plane - HOT_PLANE, 0), per)
    gathers_hot = jnp.logical_and(plane == 0, me < 2)
    n_sources = jnp.where(me == 0, n_dp * per, n_dp * (n_tp - HOT_PLANE - per))

    def block(tp, start=0, size=n_pos):
        return pl.ds(pl.multiple_of(tp * n_pos + start, 8), size)

    barrier = greet([{"tp": lax.rem(plane + i, n_tp)} for i in range(1, n_tp)]
                    + [{"dp": lax.rem(me + i, n_dp)} for i in range(1, n_dp)])

    @pl.when(is_hot)
    def _():
        pl.semaphore_signal(barrier, inc=1, device_id={"dp": owner, "tp": 0}, device_id_type=MESH)

    @pl.when(gathers_hot)
    def _():
        @pl.loop(0, n_sources)
        def _(k):
            tp = HOT_PLANE + per * me + lax.div(k, n_dp)
            pl.semaphore_signal(barrier, inc=1, device_id={"dp": lax.rem(k, n_dp), "tp": tp}, device_id_type=MESH)

    extra = jnp.where(is_hot, 1, 0) + jnp.where(gathers_hot, n_sources, 0)
    pl.semaphore_wait(barrier, n_dp + n_tp - 2 + extra)

    def peer(i):
        return lax.rem(me + i, n_dp), lax.rem(me + n_dp - i, n_dp)

    def cols_of(c):
        return pl.ds(pl.multiple_of(c * wide, 128), wide)

    def idx_copy(i, to, slot):
        return pltpu.make_async_remote_copy(
            src_ref=send_ref.at[lax.div(to, 2)], dst_ref=idx_ref.at[slot], send_sem=i_send.at[i], recv_sem=i_recv.at[i],
            device_id={"dp": to}, device_id_type=MESH)

    for i in range(1, n_dp):
        idx_copy(i, peer(i)[0], me).start()

    def to_partner(k, c):
        return tp_copy(send.at[pl.ds(k * n_pos, n_pos), cols_of(c)], chip_sum.at[k, :, cols_of(c)],
                       (d_send, d_recv), (k, c), line.partner)

    def look_up(k):
        mine_tp = line.chips[order[k]]
        for part, tp in enumerate((line.other(mine_tp), mine_tp)):
            lanes = lax.broadcasted_iota(I32, (n_pos, sel.shape[1]), 1)
            sel[pl.ds(part * n_pos, n_pos), :] = (lanes == comb_ref[block(tp), :1]).astype(BF16)

        @pl.loop(0, NCHUNK)
        def _(c):
            cols = cols_of(c)
            rows = jnp.dot(sel[:, :FRONT], front_ref[:, cols], preferred_element_type=F32)
            rows = (rows + jnp.dot(sel[:, FRONT:], far_ref[:, cols], preferred_element_type=F32)) * scale
            send[pl.ds(k * n_pos, n_pos), cols] = rows[:n_pos]
            mine[k, :, cols] = rows[n_pos:]
            to_partner(k, c).start()

    def add_chip(k, c):
        to_partner(k, c).wait_recv()
        chip_sum[k, :, cols_of(c)] += mine[k, :, cols_of(c)]

    def half_copy(side, c):
        return tp_copy(chip_sum.at[0, pl.ds(side * half, half), cols_of(c)], half_in.at[side, :, cols_of(c)],
                       (h_send, h_recv), (side, c), (line.right, line.left)[side])

    def full_copy(side, part, c):
        rows = pl.ds(part * half, half)
        return tp_copy(chip_sum.at[1 + side, rows, cols_of(c)], full_in.at[side, rows, cols_of(c)],
                       (f_send, f_recv), (2 * side + part, c), (line.right, line.left)[side])

    look_up(0)

    @pl.loop(0, NCHUNK)
    def _(c):
        add_chip(0, c)
        for side in range(2):
            half_copy(side, c).start()

    look_up(1)
    look_up(2)

    @pl.loop(0, NCHUNK)
    def _(c):
        add_chip(1, c)
        full_copy(0, 1, c).start()
        add_chip(2, c)
        full_copy(1, 0, c).start()

    @pl.loop(0, NCHUNK)
    def _(c):
        for side in range(2):
            half_copy(side, c).wait_recv()
            chip_sum[1 + side, pl.ds(side * half, half), cols_of(c)] += half_in[side, :, cols_of(c)]
            full_copy(side, side, c).start()

    look_up(3)

    def n_rows(blk):
        return hot_rows(plane) + cold_cap(plane, blk)

    @pl.loop(0, SLOTS // 128)
    def _(b):
        base = pl.multiple_of(b * 128, 128)
        rows = lax.broadcasted_iota(I32, (128, n_tok), 0) + base
        pick[pl.ds(base, 128), :] = (rows == slot_ref[...]).astype(BF16)

    @pl.loop(0, n_dp)
    def _(s):
        @pl.loop(lax.div(n_rows(me), 8), STRIDE // 8)
        def _(r):
            recv[s, pl.ds(pl.multiple_of(r * 8, 8), 8), :] = jnp.zeros((8, dim), F32)

    idx_ref[pl.ds(me, 1)] = send_ref[pl.ds(lax.div(me, 2), 1)]
    for i in range(1, n_dp):
        to, frm = peer(i)
        idx_copy(i, to, me).wait_send()
        idx_copy(i, frm, frm).wait_recv()

    flag_ref[...] = jnp.max(idx_ref[...], axis=0)

    @pl.loop(0, n_dp // 2)
    def _(p):
        upper = lax.broadcasted_iota(I32, (1, 128), 1) >= STRIDE
        here = (lax.rem(me, 2) == 1)

        def for_me(s):
            v = idx_ref[s, 0:1, :]
            return jnp.where(jnp.logical_xor(upper, here), pltpu.roll(v, STRIDE, 1), v)

        idx = jnp.where(upper, for_me(2 * p + 1), for_me(2 * p))
        rows = lax.broadcasted_iota(I32, (place.shape[0], 128), 0)
        place[:, pl.ds(pl.multiple_of(p * 128, 128), 128)] = (rows == idx).astype(BF16)

    gain = 1.0 + gain_ref[...]
    w_acc[...] = jnp.zeros(w_acc.shape, F32)

    @pl.loop(0, NCHUNK)
    def _(c):
        add_chip(3, c)
        for side in range(2):
            for part in range(2):
                full_copy(side, part, c).wait_recv()

        for k in range(4):
            to_partner(k, c).wait_send()

    @pl.loop(0, n_pos // 16)
    def _(q):
        for r in range(2):
            rows = pl.ds(pl.multiple_of(q * 16 + r * 8, 8), 8)
            total = (chip_sum[3, rows, :] + full_in[0, rows, :]) + full_in[1, rows, :]
            x_emb = total.astype(BF16)
            x_ref[rows, :] = x_emb
            x = x_emb.astype(F32)
            r_inv = lax.rsqrt(jnp.mean(x * x, axis=-1, keepdims=True) + NORM_EPS)
            x_hat = x * r_inv
            y_ref[rows, :] = (x_hat * gain).astype(BF16)
            dy = dyn_ref[rows, :].astype(F32)
            a = dy * gain
            g_ref[rows, :] = dyr_ref[rows, :].astype(F32) + r_inv * (a - x_hat * jnp.mean(a * x_hat, axis=-1, keepdims=True))
            w_acc[...] += dy * x_hat

    w_part[...] = jnp.sum(w_acc[...], axis=0, keepdims=True)

    def ag_sent(kind, c):
        cols = cols_of(c)
        rows, to = (
            (block(plane), line.right), (block(plane), line.left),
            (block(line.left, 0, half), line.right), (block(line.right, half, half), line.left),
            (block(plane), line.partner), (block(line.left), line.partner),
            (block(line.right), line.partner), (block(line.opp), line.partner))[kind]
        src = g_ref.at[:, cols] if kind in (0, 1, 4) else g_all.at[rows, cols]
        return tp_copy(src, g_all.at[rows, cols], (ag_send, ag_recv), (kind, c), to)

    def ag_arrives(kind, c):
        cols = cols_of(c)
        rows = (block(line.left), block(line.right),
                block(line.opp, 0, half), block(line.opp, half, half),
                block(line.partner), block(line.other(line.left)),
                block(line.other(line.right)), block(line.other(line.opp)))[kind]
        return tp_copy(g_all.at[rows, cols], g_all.at[rows, cols], (ag_send, ag_recv), (kind, c), line.partner)

    def w_copy(i, slot):
        return pltpu.make_async_remote_copy(
            src_ref=w_part, dst_ref=w_dp.at[slot], send_sem=wd_send.at[i], recv_sem=wd_recv.at[i],
            device_id={"dp": peer(i)[0]}, device_id_type=MESH)

    def wt_copy(i, slot):
        return tp_copy(w_sum, w_tp.at[slot], (wt_send, wt_recv), i, lax.rem(plane + i, n_tp))

    def row_copy(c, i, size, to, slot):
        return pltpu.make_async_remote_copy(
            src_ref=send.at[pl.ds(pl.multiple_of(slot_base(plane, to), 8), size), cols_of(c)],
            dst_ref=recv.at[slot, pl.ds(0, size), cols_of(c)],
            send_sem=a_send.at[c, i], recv_sem=a_recv.at[c, i],
            device_id={"dp": to}, device_id_type=MESH)

    def by_size(want, fn):
        for size in sizes:
            @pl.when(want == size)
            def _():
                fn(size)

    at = pl.multiple_of(lax.rem(jnp.maximum(plane - HOT_PLANE, 0), per) * (n_dp * HOT_ROWS) + me * HOT_ROWS, 8)

    def hot_copy(c):
        return pltpu.make_async_remote_copy(
            src_ref=hot_send.at[:, cols_of(c)], dst_ref=hot_recv.at[pl.ds(at, HOT_ROWS), cols_of(c)],
            send_sem=hot_out.at[c], recv_sem=hot_in.at[0],
            device_id={"dp": owner, "tp": 0}, device_id_type=MESH)

    def send_own(c):
        for kind in (0, 1, 4):
            ag_sent(kind, c).start()

    send_own(0)
    send_own(1)
    for i in range(1, n_dp):
        w_copy(i, me).start()
    g_all[block(plane), :] = g_ref[...]

    @pl.loop(0, NCHUNK + 2 + LAG)
    def _(i):
        @pl.when(i + 2 < NCHUNK)
        def _():
            send_own(i + 2)

        @pl.when(i < NCHUNK)
        def _():
            ag_arrives(0, i).wait_recv()
            ag_sent(2, i).start()
            ag_sent(5, i).start()
            ag_arrives(1, i).wait_recv()
            ag_sent(3, i).start()
            ag_sent(6, i).start()

        @pl.when(jnp.logical_and(i >= 1, i < NCHUNK + 1))
        def _():
            ag_arrives(2, i - 1).wait_recv()
            ag_arrives(3, i - 1).wait_recv()
            ag_sent(7, i - 1).start()

        @pl.when(jnp.logical_and(i >= 2, i < NCHUNK + 2))
        def _():
            c = i - 2
            for kind in (4, 5, 6, 7):
                ag_arrives(kind, c).wait_recv()
            cols = cols_of(c)
            send[:, cols] = dot_exact(pick[...], g_all[:, cols])

            @pl.loop(1, n_dp)
            def _(k):
                to = peer(k)[0]
                by_size(n_rows(to), lambda size: row_copy(c, k, size, to, me).start())

            def keep(size):
                recv[pl.ds(me, 1), :size, cols] = send[pl.ds(pl.multiple_of(slot_base(plane, me), 8), size), cols][None]

            by_size(n_rows(me), keep)

        @pl.when(i == 3)
        def _():
            w_dp[pl.ds(me, 1)] = w_part[...][None]
            for k in range(1, n_dp):
                w_copy(k, me).wait_send()
                w_copy(k, peer(k)[1]).wait_recv()
            w_sum[...] = jnp.sum(w_dp[...], axis=0)
            for k in range(1, n_tp):
                wt_copy(k, plane).start()
            w_tp[pl.ds(plane, 1)] = w_sum[...][None]

        @pl.when(i >= 2 + LAG)
        def _():
            c = i - 2 - LAG

            @pl.loop(1, n_dp)
            def _(k):
                to, frm = peer(k)
                by_size(n_rows(to), lambda size: row_copy(c, k, size, to, me).wait_send())
                by_size(n_rows(me), lambda size: row_copy(c, k, size, frm, frm).wait_recv())

            cols = cols_of(c)
            rows = recv[:, :, cols]

            @pl.when(is_hot)
            def _():
                hot_send[:, cols] = jnp.sum(rows[:, :HOT_ROWS, :], axis=0) * scale
                hot_copy(c).start()

            out_ref[:, cols] = dot_exact(place[...], rows.reshape(n_slots, wide)) * scale

    for i in range(1, n_tp):
        wt_copy(i, plane).wait_send()
        wt_copy(i, lax.rem(plane + n_tp - i, n_tp)).wait_recv()
    wout_ref[...] = jnp.sum(w_tp[...], axis=0)

    @pl.loop(0, NCHUNK)
    def _(c):
        for side in range(2):
            half_copy(side, c).wait_send()
            for part in range(2):
                full_copy(side, part, c).wait_send()

    @pl.loop(0, NCHUNK)
    def _(c):
        for kind in range(8):
            ag_sent(kind, c).wait_send()

    @pl.when(is_hot)
    def _():
        @pl.loop(0, NCHUNK)
        def _(c):
            hot_copy(c).wait_send()

    def take_hot(n):
        ref = hot_recv.at[pl.ds(0, n), :]
        pltpu.make_async_remote_copy(
            src_ref=ref, dst_ref=ref, send_sem=hot_out.at[0], recv_sem=hot_in.at[0],
            device_id={"dp": 2, "tp": 0}, device_id_type=MESH).wait_recv()
        out_ref[pl.ds(0, n), :] += hot_recv[pl.ds(0, n), :]

    total = hot_recv.shape[0]

    @pl.when(jnp.logical_and(plane == 0, me == 0))
    def _():
        take_hot(total)

    @pl.when(jnp.logical_and(plane == 0, me == 1))
    def _():
        take_hot(HOT - total)


def fused_step(n_dp, n_tp, out_rows, comb, far, table, slot, send_idx, w_norm, dy_norm, dy_resid):
    n_pos, dim = dy_norm.shape
    n_tok = n_pos * n_tp
    half = n_pos // 2
    dma = pltpu.SemaphoreType.DMA
    vmem = pl.BlockSpec(memory_space=VMEM)
    shape = jax.ShapeDtypeStruct
    return pl.pallas_call(
        functools.partial(step_kernel, n_dp, n_tp),
        grid=(1,),
        out_shape=(shape((n_pos, dim), BF16), shape((n_pos, dim), BF16),
                   shape((out_rows, dim), F32), shape((1, dim), F32), shape((8, 128), I32)),
        in_specs=[vmem, vmem, pl.BlockSpec((FRONT, dim), lambda i: (0, 0), pipeline_mode=pl.Buffered(1))] + [vmem] * 5,
        out_specs=(vmem,) * 5,
        scratch_shapes=[
            VMEM((n_dp, 8, 128), I32),
            VMEM((2 * n_pos, FRONT + 2 * FAR), BF16),
            VMEM((4, n_pos, dim), F32),
            VMEM((4, n_pos, dim), F32),
            VMEM((2, half, dim), F32),
            VMEM((2, n_pos, dim), F32),
            VMEM((n_pos, dim), F32),
            VMEM((n_tok, dim), F32),
            VMEM((SLOTS, n_tok), BF16),
            VMEM((out_rows, n_dp * STRIDE), BF16),
            VMEM((SLOTS, dim), F32),
            VMEM((n_dp, STRIDE, dim), F32),
            VMEM((HOT_ROWS, dim), F32),
            VMEM((out_rows, dim), F32),
            VMEM((8, dim), F32),
            VMEM((1, dim), F32),
            VMEM((n_dp, 1, dim), F32),
            VMEM((1, dim), F32),
            VMEM((n_tp, 1, dim), F32),
            dma((4, NCHUNK)), dma((4, NCHUNK)), dma((2, NCHUNK)), dma((2, NCHUNK)),
            dma((4, NCHUNK)), dma((4, NCHUNK)), dma((n_dp,)), dma((n_dp,)),
            dma((8, NCHUNK)), dma((8, NCHUNK)),
            dma((NCHUNK, n_dp)), dma((NCHUNK, n_dp)), dma((NCHUNK,)), dma((1,)),
            dma((n_dp,)), dma((n_dp,)), dma((n_tp,)), dma((n_tp,)),
        ],
        compiler_params=pltpu.CompilerParams(collective_id=1, has_side_effects=True, vmem_limit_bytes=67043328),
        name="fused_step",
    )(comb, far, table, slot, send_idx, w_norm.reshape(1, dim), dy_norm, dy_resid)


def swap(x, axis):
    return lax.all_to_all(x, axis, split_axis=0, concat_axis=0)


def dense_step(n_dp, n_tp, out_rows, ids, table, w_norm, dy_norm, dy_resid):
    dim = table.shape[1]
    rows = table.shape[0]
    scale = math.sqrt(dim)
    local = ids - lax.axis_index("tp") * rows
    owned = (local >= 0) & (local < rows)
    looked = jnp.take(table, jnp.where(owned, local, 0), axis=0).astype(F32) * scale
    part = jnp.where(owned[:, None], looked, 0.0).reshape((n_tp,) + dy_norm.shape)
    x_emb = jnp.sum(swap(part, "tp"), axis=0).astype(BF16)
    x = x_emb.astype(F32)
    r_inv = lax.rsqrt(jnp.mean(x * x, axis=-1, keepdims=True) + NORM_EPS)
    x_hat = x * r_inv
    gain = 1.0 + w_norm
    y_norm = (x_hat * gain).astype(BF16)
    dy = dy_norm.astype(F32)
    a = dy * gain
    g = dy_resid.astype(F32) + r_inv * (a - x_hat * jnp.mean(a * x_hat, axis=-1, keepdims=True))
    w = jnp.sum(dy * x_hat, axis=0)[None]
    w = jnp.sum(swap(jnp.broadcast_to(w, (n_dp,) + w.shape), "dp"), axis=0)
    w = jnp.sum(swap(jnp.broadcast_to(w, (n_tp,) + w.shape), "tp"), axis=0)
    g_all = swap(jnp.broadcast_to(g, (n_tp,) + g.shape), "tp").reshape(-1, dim)
    shard = jax.ops.segment_sum(g_all, jnp.where(owned, local, rows), num_segments=rows, mode="drop")
    emb = jnp.sum(swap(shard.reshape(n_dp, out_rows, -1), "dp"), axis=0) * scale
    return x_emb, y_norm, emb, w


def solution(mesh):
    n_dp, n_tp = mesh.shape["dp"], mesh.shape["tp"]

    def local_step(tokens, emb_table, w_norm, dy_norm, dy_resid):
        out_rows = emb_table.shape[0] // n_dp
        ids = tokens[0]
        comb, far, slot, send_idx = make_plan(n_dp, n_tp, tokens, emb_table)
        *fast, w_fast, flag = fused_step(n_dp, n_tp, out_rows, comb, far, emb_table, slot, send_idx, w_norm, dy_norm[0], dy_resid[0])
        fits = flag[1, 0] == 0
        x_emb, y_norm, emb_grad, w_sum = lax.cond(
            fits,
            lambda: (*hand_on(*fast), w_fast),
            lambda: dense_step(n_dp, n_tp, out_rows, ids, emb_table, w_norm, dy_norm[0], dy_resid[0]),
        )
        return x_emb[None], y_norm[None], emb_grad, w_sum[0]

    act_spec = P("dp", "tp", None)
    return jax.shard_map(local_step, mesh=mesh, in_specs=(P("dp", None), P("tp", None), P(None), act_spec, act_spec), out_specs=(act_spec, act_spec, P(("tp", "dp"), None), P(None)), check_vma=False)
```
